32 devices in a mesh: blk: 8 (over y, x, core), width: 4 (over z).
Axes of the slice: x: 2, y: 2, z: 4, core: 2. Of those that a mesh axis runs over, the one named last changes fastest.
Arguments:
- inputs: bfloat16 [8, 128, 2048], P('blk', None, 'width'), may hold values from -6 to 6
- encoder: bfloat16 [8, 2048, 4096], P('blk', 'width'), may hold values from -0.125 to 0.125
- enc_bias: float32 [8, 4096], P('blk'), may hold values from -3 to 3
- active_blocks: int32 [8, 128, 32], P('blk'), may hold values 0 or 1
- near_decoders: bfloat16 [8, 4, 4096, 2048], P('blk', None, None, 'width'), may hold values from -0.09375 to 0.09375
- far_decoders: bfloat16 [8, 2048, 2048], P('blk', None, 'width'), may hold values from -0.09375 to 0.09375
- targets: bfloat16 [8, 128, 2048], P('blk', None, 'width'), may hold values from -6 to 6
Outputs:
- reconstruction: float32 [8, 128, 2048], P('blk', None, 'width')
- grad_encoder: bfloat16 [8, 2048, 4096], P('blk', 'width')
- grad_bias: float32 [8, 4096], P('blk')
The draws below stay inside these ranges and needn't reach their ends.
All inputs are finite; a program needn't handle non-finite values. No bound on the sum of `active_blocks` on one device may be relied on, other than what follows from the above.
Results may differ from the reference program's by a relative error of at most 0.011.
Values may be sent and summed in bfloat16 or wider, within the bound.
A program may use at most 128 MiB of HBM per device.

```python
import jax
import jax.numpy as jnp

D = 2048
F = 4096
FBLK = 128
TOK = 128
LAYERS = 8
NEAR = 4
FB = 32


def plant(values, rng, smallest, largest):
    place = [jax.random.randint(jax.random.fold_in(rng, axis), (), 0, length) for axis, length in enumerate(values.shape)]
    main_axis = values.shape.index(max(values.shape))
    neighbour = place[:main_axis] + [(place[main_axis] + 1) % values.shape[main_axis]] + place[main_axis + 1:]
    return values.at[tuple(place)].set(smallest).at[tuple(neighbour)].set(largest)


def block_levels(stream_key, shape, split, least, high):
    level, own = 1.0, jax.random.fold_in(stream_key, 6)
    for dim, shards_of in split:
        heights = jnp.exp(jax.random.uniform(jax.random.fold_in(own, dim), (shards_of,), jnp.float32, least / len(split), high / len(split)))
        level = level * jnp.repeat(heights, shape[dim] // shards_of).reshape([-1 if axis == dim else 1 for axis in range(len(shape))])
    return level


def gaussian(own_key, dims, width, reach, shards=(), kind=jnp.bfloat16):
    entries = width * jax.random.normal(own_key, dims, jnp.float32)
    if shards:
        entries = entries * block_levels(own_key, dims, shards, -0.22, 0.18)
    return jnp.clip(entries, -reach, reach).astype(kind)


def setup_inputs(seed: int = 0) -> dict:
    arg_keys = jax.random.split(jax.random.key(seed), 8)
    inputs = gaussian(arg_keys[0], (LAYERS, TOK, D), 1.0, 6.0, ((0, 8), (2, 4)))
    encoder = gaussian(arg_keys[1], (LAYERS, D, F), D ** -0.5, 0.125, ((0, 8), (1, 4)))
    enc_bias = gaussian(arg_keys[2], (LAYERS, F), 0.5, 3.0, ((0, 8),), jnp.float32)
    active_blocks = plant((jax.random.randint(arg_keys[3], (LAYERS, TOK, FB), 0, 2) < 1).astype(jnp.int32), jax.random.fold_in(arg_keys[3], 1), 0, 1)
    near_decoders = gaussian(arg_keys[4], (LAYERS, NEAR, F, D), F ** -0.5, 0.09375, ((0, 8), (3, 4)))
    far_decoders = gaussian(arg_keys[5], (LAYERS, F // 2, D), F ** -0.5, 0.09375, ((0, 8), (2, 4)))
    targets = gaussian(arg_keys[6], (LAYERS, TOK, D), 1.0, 6.0, ((0, 8), (2, 4)))
    return {"inputs": inputs, "encoder": encoder, "enc_bias": enc_bias, "active_blocks": active_blocks, "near_decoders": near_decoders, "far_decoders": far_decoders, "targets": targets}


def expand_mask(blocks):
    return jnp.repeat(blocks.astype(jnp.float32), FBLK, axis=-1)


def pair_decoder(near_decoders, far_decoders, lower, upper):
    layers = LAYERS
    near_count = layers // 2
    spread = upper - lower
    if spread < near_count:
        return near_decoders[upper, spread]
    if spread == near_count:
        return jnp.concatenate([far_decoders[lower], far_decoders[upper]], axis=0)
    return near_decoders[lower, lower + layers - upper]


def reference(inputs, encoder, enc_bias, active_blocks, near_decoders, far_decoders, targets):
    layers = LAYERS
    masks_all = [expand_mask(active_blocks[level]) for level in range(layers)]
    activations = []
    for level in range(layers):
        pre_value = jnp.dot(inputs[level], encoder[level], preferred_element_type=jnp.float32) + enc_bias[level]
        activations.append((masks_all[level] * pre_value).astype(jnp.bfloat16))
    recon_rows = []
    out_grads = []
    for upper in range(layers):
        total = jnp.zeros((TOK, D), jnp.float32)
        for lower in range(upper + 1):
            weights = pair_decoder(near_decoders, far_decoders, lower, upper)
            total = total + jnp.dot(activations[lower], weights, preferred_element_type=jnp.float32)
        recon_rows.append(total)
        out_grads.append((total - targets[upper].astype(jnp.float32)).astype(jnp.bfloat16))
    enc_grads = []
    bias_grads = []
    for lower in range(layers):
        total = jnp.zeros((TOK, F), jnp.float32)
        for upper in range(lower, layers):
            weights = pair_decoder(near_decoders, far_decoders, lower, upper)
            total = total + jnp.dot(out_grads[upper], weights.T, preferred_element_type=jnp.float32)
        pre_grad = (masks_all[lower] * total).astype(jnp.bfloat16)
        enc_grads.append(jnp.dot(inputs[lower].T, pre_grad, preferred_element_type=jnp.float32).astype(jnp.bfloat16))
        bias_grads.append(jnp.sum(pre_grad.astype(jnp.float32), axis=0))
    return jnp.stack(recon_rows), jnp.stack(enc_grads), jnp.stack(bias_grads)
```

```python
import functools

import jax
import jax.numpy as jnp
from jax import lax
from jax.experimental import pallas as pl
from jax.experimental.pallas import tpu as pltpu
from jax.sharding import PartitionSpec as P

BF = jnp.bfloat16
F32 = jnp.float32


def dot(a, b):
    return jnp.dot(a, b, preferred_element_type=F32)


def dot_t(a, b):
    return lax.dot_general(a, b, (((1,), (1,)), ((), ())), preferred_element_type=F32)


def step_kernel(B, W, C, FBLK, x_ref, enc_hbm, bias_ref, blocks_ref, near_hbm, far_hbm, tgt_ref,
                recon_ref, pg_ref, gb_ref,
                enc, near, far, z_out, z_in, acts, p_acc, p_out, p_in, og, terms, duo, ret, rel, own, mask, gb,
                enc_sem, near_sem, far_sem, z_s, z_r, ad_s, af_s, a_r, p_s, p_r, o_s, o_r,
                d_s, d_r, r_s, r_r, l_s, l_r, g_s, g_r):
    N = B // 2
    G = mask.shape[0]
    H = G // 2
    ROOT = W // 2
    b = lax.axis_index("blk")
    w = lax.axis_index("width")
    even = lax.rem(b, 2) == 0
    odd = lax.rem(b, 2) == 1
    relay = N == 4
    mid = (b >= N - 2) & (b < N) & relay
    top = (b >= B - 2) & relay
    far_side = (b >= N) & (b < B - 2) & relay
    not_mid = jnp.logical_not(mid)
    not_top = jnp.logical_not(top)
    not_far_side = jnp.logical_not(far_side)
    chip = lax.div(b, 2)
    late = 2 * (lax.div(chip, 2) - lax.div(chip, 3)) if relay else 0

    def col(j):
        return pl.ds(pl.multiple_of(j * C, C), C)

    def remote(src, dst, s, r, to_b, to_w):
        return pltpu.make_async_remote_copy(src_ref=src, dst_ref=dst, send_sem=s, recv_sem=r,
                                            device_id=(to_b, to_w), device_id_type=pl.DeviceIdType.MESH)

    def loop(lo, hi, body):
        def run(i, carry):
            body(i)
            return carry
        lax.fori_loop(lo, hi, run, 0)

    def inside(j):
        return (j >= 0) & (j < G)

    def enc_copy(j):
        return pltpu.make_async_copy(enc_hbm.at[:, col(j)], enc.at[:, col(j)], enc_sem.at[j])

    def near_copy(k):
        return pltpu.make_async_copy(near_hbm.at[k], near.at[k], near_sem.at[k])

    far_copy = pltpu.make_async_copy(far_hbm, far, far_sem)

    def z_copy(lane, j, to):
        return remote(z_out.at[lane, j], z_in.at[lane, j], z_s.at[lane, j], z_r.at[lane, j], b, to)

    def act_direct(k, j):
        return remote(acts.at[0, j], acts.at[k, j], ad_s.at[k, j], a_r.at[k, j], b + k, w)

    def act_pass(k_from, k, j, to):
        return remote(acts.at[k_from, j], acts.at[k, j], af_s.at[k, j], a_r.at[k, j], to, w)

    def share(k):
        return remote(p_out.at[k], p_in.at[k], p_s.at[k], p_r.at[k], b - k + B, w)

    def out_grad(k):
        return remote(og.at[0], og.at[k], o_s.at[k], o_r.at[k], b + k - B, w)

    def duo_copy(k_from, k, j, to):
        return remote(terms.at[k_from, j], duo.at[k, j], d_s.at[k_from, j], d_r.at[k, j], to, w)

    def ret_copy(k_from, k, j, to):
        return remote(terms.at[k_from, j], ret.at[k, j], r_s.at[k_from, j], r_r.at[k, j], to, w)

    def rel_copy(j):
        return remote(terms.at[2, j], rel.at[j], l_s.at[j], l_r.at[j], b + 2, w)

    def bias_copy(d):
        return remote(gb, gb, g_s.at[d], g_r, b, lax.rem(w + d, W))

    loop(0, G, lambda j: enc_copy(j).start())

    barrier = pltpu.get_barrier_semaphore()
    for d in range(1, W):
        pl.semaphore_signal(barrier, inc=1, device_id=(b, lax.rem(w + d, W)), device_id_type=pl.DeviceIdType.MESH)
    for d in range(1, B):
        pl.semaphore_signal(barrier, inc=1, device_id=(lax.rem(b + d, B), w), device_id_type=pl.DeviceIdType.MESH)

    fb = blocks_ref.shape[0]
    active = blocks_ref[...].astype(F32).astype(BF)
    row_id = lax.broadcasted_iota(jnp.int32, (fb, C), 0)
    lane_id = lax.broadcasted_iota(jnp.int32, (fb, C), 1) // FBLK

    def masks(j):
        spread = jnp.where(row_id - j * (C // FBLK) == lane_id, 1.0, 0.0).astype(BF)
        mask[j] = lax.dot_general(active, spread, (((0,), (0,)), ((), ())), preferred_element_type=F32).astype(BF)

    loop(0, G, masks)
    recon_ref[...] = jnp.zeros(recon_ref.shape, F32)
    p_acc[...] = jnp.zeros(p_acc.shape, F32)
    pl.semaphore_wait(barrier, W + B - 2)

    def ends(phase, j):
        @pl.when(w == 0)
        def _():
            z_out[2 * phase, j] = own[j].astype(BF)
            z_copy(2 * phase, j, w + 1).start()

        @pl.when(w == W - 1)
        def _():
            z_out[2 * phase + 1, j] = own[j].astype(BF)
            z_copy(2 * phase + 1, j, w - 1).start()

    def first(j):
        enc_copy(j).wait()
        own[j] = dot(x_ref[...], enc[:, col(j)])
        ends(0, j)

    loop(0, G, first)
    for k in range(N):
        near_copy(k).start()
    far_copy.start()

    def hop(phase, t):
        up = t - w + 1
        down = t - (W - 2) + w

        @pl.when((w > 0) & inside(up))
        def _():
            z_copy(2 * phase, up, w).wait_recv()

            @pl.when(w < W - 1)
            def _():
                z_out[2 * phase, up] = (own[up] + z_in[2 * phase, up].astype(F32)).astype(BF)
                z_copy(2 * phase, up, w + 1).start()

        @pl.when((w < W - 1) & inside(down))
        def _():
            z_copy(2 * phase + 1, down, w).wait_recv()

            @pl.when(w > 0)
            def _():
                z_out[2 * phase + 1, down] = (own[down] + z_in[2 * phase + 1, down].astype(F32)).astype(BF)
                z_copy(2 * phase + 1, down, w - 1).start()

    def total(phase, j, put):
        @pl.when(w == 0)
        def _():
            put(own[j] + z_in[2 * phase + 1, j].astype(F32))

        @pl.when(w == W - 1)
        def _():
            put(own[j] + z_in[2 * phase, j].astype(F32))

        @pl.when((w > 0) & (w < W - 1))
        def _():
            put(own[j] + z_in[2 * phase, j].astype(F32) + z_in[2 * phase + 1, j].astype(F32))

    def act_sends(j, act):
        for k in range(2, N, 2):
            @pl.when((b + k < B) & not_mid)
            def _():
                act(act_direct(k, j))

        @pl.when(even)
        def _():
            act(act_pass(0, 1, j, b + 1))

        @pl.when(odd & (b + N - 1 < B) & not_mid)
        def _():
            act(act_direct(N - 1, j))

        @pl.when(mid | (even & (b + N < B) & (j >= H)))
        def _():
            act(act_direct(N, j))

    start = lambda c: c.start()
    end = lambda c: c.wait_send()

    def finish(j):
        def put(value):
            acts[0, j] = (mask[j].astype(F32) * (value + bias_ref[:, col(j)])).astype(BF)

        total(0, j, put)
        act_sends(j, start)
        recon_ref[...] += dot(acts[0, j], near[0, col(j), :])
        for k in range(1, N):
            @pl.when(b < k)
            def _():
                p_acc[k] += dot(acts[0, j], near[k, col(j), :])

        @pl.when((b < N) & (j < H))
        def _():
            p_acc[N] += dot(acts[0, j], far[col(j), :])

    def inside_term(k, j):
        if k < N:
            recon_ref[...] += dot(acts[k, j], near[k, col(j), :])
        else:
            recon_ref[...] += dot(acts[k, j], far[col(j - H), :])

    def act_forwards(k, j, act):
        if k % 2 == 0 and k < N:
            @pl.when(even)
            def _():
                act(act_pass(k, k + 1, j, b + 1))

            @pl.when(odd)
            def _():
                act(act_pass(k, k - 1, j, b - 1))
        if k == N - 1:
            @pl.when(j >= H)
            def _():
                act(act_pass(k, N, j, b + 1))

    def arrival(k, j):
        return remote(acts.at[k, j], acts.at[k, j], ad_s.at[k, j], a_r.at[k, j], b, w)

    def relay_sends(j, act):
        act(act_pass(N, 2, j, b - 2))

        @pl.when(odd)
        def _():
            act(act_pass(N, N - 1, j, b - 1))

    def inner(j):
        if relay:
            @pl.when(top)
            def _():
                arrival(N, j).wait_recv()
                relay_sends(j, start)

                @pl.when(j >= H)
                def _():
                    inside_term(N, j)
        for k in list(range(2, N, 2)) + [N - 1, N]:
            cond = b >= k
            if k >= N - 1:
                cond = cond & even & not_top
            if k == N:
                cond = cond & (j >= H)

            @pl.when(cond)
            def _():
                arrival(k, j).wait_recv()
                act_forwards(k, j, start)
                inside_term(k, j)

    def passed(j):
        for k in list(range(1, N, 2)) + [N]:
            cond = b >= k
            if k == N - 1:
                cond = cond & (odd | top)
            if k == N:
                cond = cond & odd & not_top
            if k == N:
                cond = cond & (j >= H)

            @pl.when(cond)
            def _():
                arrival(k, j).wait_recv()
                inside_term(k, j)

    AHEAD, BEHIND = 3, 3

    def forward(t):
        hop(0, t)
        f = t - (W - 2)

        @pl.when(f == 0)
        def _():
            for k in range(N):
                near_copy(k).wait()
            far_copy.wait()

        @pl.when(inside(f))
        def _():
            finish(f)

        for k in range(1, N + 1):
            @pl.when((f == G - 1) & (b < k))
            def _():
                p_out[k] = p_acc[k].astype(BF)
                share(k).start()

        i = f - AHEAD - late

        @pl.when(inside(i))
        def _():
            inner(i)

        p = i - BEHIND

        @pl.when(inside(p))
        def _():
            passed(p)

    loop(0, G + W - 2 + AHEAD + BEHIND + (2 if relay else 0), forward)
    for k in range(1, N + 1):
        @pl.when(b + k >= B)
        def _():
            remote(p_out.at[k], p_in.at[k], p_s.at[k], p_r.at[k], b, w).wait_recv()
            recon_ref[...] += p_in[k].astype(F32)

    og[0] = (recon_ref[...] - tgt_ref[...].astype(F32)).astype(BF)
    for k in range(1, N + 1):
        @pl.when(b + k >= B)
        def _():
            out_grad(k).start()

    def back(j):
        for k in list(range(1, N, 2)) + [N] + list(range(2, N, 2)):
            cond = b >= k
            if k == N:
                cond = cond & (j >= H)

            @pl.when(cond)
            def _():
                rows = near[k, col(j), :] if k < N else far[col(j - H), :]
                terms[k, j] = dot_t(og[0], rows).astype(BF)
                duo_sends(k, j, start)

    def duo_sends(k, j, act):
        if k % 2 == 1 and k <= N - 3:
            @pl.when(even)
            def _():
                act(duo_copy(k, k + 1, j, b + 1))
        if k == 1:
            @pl.when(odd)
            def _():
                act(ret_copy(1, 1, j, b - 1))
        if k % 2 == 1 and k >= 3:
            @pl.when(odd)
            def _():
                act(duo_copy(k, k - 1, j, b - 1))
        if k == N - 1 and relay:
            @pl.when(even & top)
            def _():
                act(duo_copy(k, k, j, b + 1))
        if k == N:
            @pl.when(odd & not_top)
            def _():
                act(duo_copy(N, N - 1, j, b - 1))

            @pl.when(even & not_top)
            def _():
                act(ret_copy(N, N, j, b - N))

    def duo_wait(k, j):
        remote(duo.at[k, j], duo.at[k, j], d_s.at[k, j], d_r.at[k, j], b, w).wait_recv()

    def duo_add(k, j):
        duo_wait(k, j)
        terms[k, j] = (terms[k, j].astype(F32) + duo[k, j].astype(F32)).astype(BF)

    def down_sends(k, j, act):
        @pl.when(not_far_side)
        def _():
            act(ret_copy(k, k, j, b - k))
        if k == 2 and relay:
            @pl.when(far_side)
            def _():
                act(rel_copy(j))

    def down(j):
        for k in range(2, N, 2):
            @pl.when(b >= k)
            def _():
                duo_add(k, j)
                down_sends(k, j, start)

        @pl.when(even & (b >= N - 1) & not_top)
        def _():
            @pl.when(j >= H)
            def _():
                duo_add(N - 1, j)
            ret_copy(N - 1, N - 1, j, b - (N - 1)).start()

    def relay_down(j):
        remote(rel.at[j], rel.at[j], l_s.at[j], l_r.at[j], b, w).wait_recv()

        def put(value):
            @pl.when(j >= H)
            def _():
                terms[N, j] = (value + terms[N, j].astype(F32)).astype(BF)

            @pl.when(j < H)
            def _():
                terms[N, j] = value.astype(BF)

        @pl.when(even)
        def _():
            put(rel[j].astype(F32))

        @pl.when(odd)
        def _():
            duo_wait(N - 1, j)
            put(rel[j].astype(F32) + duo[N - 1, j].astype(F32))

        ret_copy(N, 2, j, b - N).start()

    def own_back(j):
        own[j] = dot_t(og[0], near[0, col(j), :])
        for k in range(1, N):
            @pl.when(b < k)
            def _():
                own[j] += dot_t(og[k], near[k, col(j), :])

        @pl.when((b < N) & (j < H))
        def _():
            own[j] += dot_t(og[N], far[col(j), :])

    def ret_add(k, j):
        remote(ret.at[k, j], ret.at[k, j], r_s.at[k, j], r_r.at[k, j], b, w).wait_recv()
        own[j] += ret[k, j].astype(F32)

    def collect(j):
        @pl.when(even)
        def _():
            ret_add(1, j)
        for k in range(2, N, 2):
            @pl.when(b + k < B)
            def _():
                ret_add(k, j)

        @pl.when(odd & (b + N - 1 < B) & not_mid)
        def _():
            ret_add(N - 1, j)

        @pl.when(even & (b + N < B) & (j >= H) & not_mid)
        def _():
            ret_add(N, j)

    def finish_back(j):
        def put(value):
            grads = (mask[j].astype(F32) * value).astype(BF)
            pg_ref[:, col(j)] = grads

            @pl.when(w == ROOT)
            def _():
                gb[:, col(j)] = jnp.sum(grads.astype(F32), axis=0, keepdims=True)

        total(1, j, put)

    DUO, RELAY, RING = 3, 6, 10

    def backward(t):
        @pl.when(t < G)
        def _():
            back(t)

        d = t - DUO

        @pl.when(inside(d))
        def _():
            down(d)

        if relay:
            r = t - RELAY

            @pl.when(top & inside(r))
            def _():
                relay_down(r)

        s = t - RING
        for k in range(1, N + 1):
            @pl.when((s == 0) & (b < k))
            def _():
                remote(og.at[k], og.at[k], o_s.at[k], o_r.at[k], b, w).wait_recv()

        @pl.when(inside(s))
        def _():
            own_back(s)
            collect(s)
            ends(1, s)

        hop(1, s)
        f = s - (W - 2)

        @pl.when(inside(f))
        def _():
            finish_back(f)

    loop(0, G + RING + W - 2, backward)

    @pl.when(w == ROOT)
    def _():
        for d in range(1, W):
            bias_copy(d).start()

    def drain(j):
        for phase in range(2):
            @pl.when(w < W - 1)
            def _():
                z_copy(2 * phase, j, w + 1).wait_send()

            @pl.when(w > 0)
            def _():
                z_copy(2 * phase + 1, j, w - 1).wait_send()
        act_sends(j, end)
        for k in list(range(2, N, 2)) + [N - 1]:
            cond = b >= k
            if k == N - 1:
                cond = cond & even & not_top

            @pl.when(cond)
            def _():
                act_forwards(k, j, end)
        if relay:
            @pl.when(top)
            def _():
                relay_sends(j, end)
                ret_copy(N, 2, j, b - N).wait_send()
        for k in range(1, N + 1):
            cond = b >= k
            if k == N:
                cond = cond & (j >= H)

            @pl.when(cond)
            def _():
                duo_sends(k, j, end)
        for k in range(2, N, 2):
            @pl.when(b >= k)
            def _():
                down_sends(k, j, end)

        @pl.when(even & (b >= N - 1) & not_top)
        def _():
            ret_copy(N - 1, N - 1, j, b - (N - 1)).wait_send()

    loop(0, G, drain)
    for k in range(1, N + 1):
        @pl.when(b < k)
        def _():
            share(k).wait_send()

        @pl.when(b + k >= B)
        def _():
            out_grad(k).wait_send()

    @pl.when(w == ROOT)
    def _():
        for d in range(1, W):
            bias_copy(d).wait_send()

    @pl.when(w != ROOT)
    def _():
        bias_copy(1).wait_recv()

    gb_ref[...] = gb[...]


def weight_kernel(x_ref, pg_ref, recon_ref, gb_ref, grad_ref, recon_out, gb_out):
    grad_ref[...] = lax.dot_general(
        x_ref[...], pg_ref[...], (((0,), (0,)), ((), ())), preferred_element_type=F32
    ).astype(BF)
    recon_out[...] = recon_ref[...]
    gb_out[...] = gb_ref[...]


def on_device(B, W, inputs, encoder, enc_bias, active_blocks, near_decoders, far_decoders, targets):
    N = B // 2
    x = inputs[0]
    tok, width = x.shape
    feats = encoder.shape[2]
    half = far_decoders.shape[1]
    out_cols = targets.shape[2]
    C = min(half, 256)
    G = feats // C
    dma = pltpu.SemaphoreType.DMA
    blocks = lambda *lead: pltpu.VMEM((*lead, tok, C), BF)
    rows = lambda *lead: pltpu.VMEM((*lead, tok, out_cols), BF)
    vmem = pl.BlockSpec(memory_space=pltpu.VMEM)
    hbm = pl.BlockSpec(memory_space=pl.ANY)
    recon, pre_grad, bias_sum = pl.pallas_call(
        functools.partial(step_kernel, B, W, C, feats // active_blocks.shape[2]),
        out_shape=(jax.ShapeDtypeStruct((tok, out_cols), F32), jax.ShapeDtypeStruct((tok, feats), BF),
                   jax.ShapeDtypeStruct((1, feats), F32)),
        in_specs=[vmem, hbm, vmem, vmem, hbm, hbm, vmem],
        out_specs=(vmem, vmem, vmem),
        scratch_shapes=[
            pltpu.VMEM((width, feats), BF),
            pltpu.VMEM((N, feats, out_cols), BF),
            pltpu.VMEM((half, out_cols), BF),
            blocks(4, G), blocks(4, G), blocks(N + 1, G),
            pltpu.VMEM((N + 1, tok, out_cols), F32),
            rows(N + 1), rows(N + 1), rows(N + 1),
            blocks(N + 1, G), blocks(N, G), blocks(N + 1, G), blocks(G),
            pltpu.VMEM((G, tok, C), F32),
            blocks(G),
            pltpu.VMEM((1, feats), F32),
            dma((G,)), dma((N,)), dma,
            dma((4, G)), dma((4, G)),
            dma((N + 1, G)), dma((N + 1, G)), dma((N + 1, G)),
            dma((N + 1,)), dma((N + 1,)), dma((N + 1,)), dma((N + 1,)),
            dma((N + 1, G)), dma((N, G)), dma((N + 1, G)), dma((N + 1, G)),
            dma((G,)), dma((G,)), dma((W,)), dma,
        ],
        compiler_params=pltpu.CompilerParams(
            collective_id=0, has_side_effects=True, vmem_limit_bytes=67_000_000),
        name="step",
    )(x, encoder[0], enc_bias, active_blocks[0].T, near_decoders[0], far_decoders[0], targets[0])
    steps = max(1, feats // 1024)
    tile = feats // steps
    part = tok // steps
    enc_grad, recon, bias_grad = pl.pallas_call(
        weight_kernel,
        grid=(steps,),
        out_shape=(jax.ShapeDtypeStruct((width, feats), BF), jax.ShapeDtypeStruct((tok, out_cols), F32),
                   jax.ShapeDtypeStruct((1, feats), F32)),
        in_specs=[pl.BlockSpec((tok, width), lambda i: (0, 0)), pl.BlockSpec((tok, tile), lambda i: (0, i)),
                  pl.BlockSpec((part, out_cols), lambda i: (i, 0)), pl.BlockSpec((1, tile), lambda i: (0, i))],
        out_specs=(pl.BlockSpec((width, tile), lambda i: (0, i)), pl.BlockSpec((part, out_cols), lambda i: (i, 0)),
                   pl.BlockSpec((1, tile), lambda i: (0, i))),
        name="weights",
    )(x, pre_grad, recon, bias_sum)
    return recon[None], enc_grad[None], bias_grad


def solution(mesh):
    return jax.shard_map(
        functools.partial(on_device, mesh.shape["blk"], mesh.shape["width"]),
        mesh=mesh,
        in_specs=(
            P("blk", None, "width"),
            P("blk", "width", None),
            P("blk", None),
            P("blk", None, None),
            P("blk", None, None, "width"),
            P("blk", None, "width"),
            P("blk", None, "width"),
        ),
        out_specs=(P("blk", None, "width"), P("blk", "width", None), P("blk", None)),
        check_vma=False,
    )
```

```python
import functools

import jax
import jax.numpy as jnp
from jax import lax
from jax.experimental import pallas as pl
from jax.experimental.pallas import tpu as pltpu
from jax.sharding import PartitionSpec as P

BF = jnp.bfloat16
F32 = jnp.float32


def dot(a, b):
    return jnp.dot(a, b, preferred_element_type=F32)


def dot_t(a, b):
    return lax.dot_general(a, b, (((1,), (1,)), ((), ())), preferred_element_type=F32)


def step_kernel(B, W, C, FBLK, x_ref, enc_hbm, bias_ref, blocks_ref, near_hbm, far_hbm, tgt_ref,
                recon_ref, pg_ref, gb_ref,
                enc, near, far, z_out, z_in, acts, p_acc, p_out, p_in, og, terms, duo, ret, rel, own, mask, gb,
                enc_sem, near_sem, far_sem, z_s, z_r, ad_s, af_s, a_r, p_s, p_r, o_s, o_r,
                d_s, d_r, r_s, r_r, l_s, l_r, g_s, g_r):
    N = B // 2
    G = own.shape[0]
    H = G // 2
    E = G // enc_sem.shape[0]
    ROOT = W // 2
    SKEW, AHEAD, LATE, BEHIND = 4, 4, 4, 4
    DUO, RELAY, RING = 3, 6, 10
    b = lax.axis_index("blk")
    w = lax.axis_index("width")
    even = lax.rem(b, 2) == 0
    odd = lax.rem(b, 2) == 1
    relay = N == 4
    mid = (b >= N - 2) & (b < N) & relay
    top = (b >= B - 2) & relay
    far_side = (b >= N) & (b < B - 2) & relay
    not_mid = jnp.logical_not(mid)
    not_top = jnp.logical_not(top)
    not_far_side = jnp.logical_not(far_side)
    chip = lax.div(b, 2)
    late = LATE * (lax.div(chip, 2) - lax.div(chip, 3)) if relay else 0

    def col(j):
        return pl.ds(pl.multiple_of(j * C, C), C)

    def remote(src, dst, s, r, to_b, to_w):
        return pltpu.make_async_remote_copy(src_ref=src, dst_ref=dst, send_sem=s, recv_sem=r,
                                            device_id=(to_b, to_w), device_id_type=pl.DeviceIdType.MESH)

    def loop(lo, hi, body):
        def run(i, carry):
            body(i)
            return carry
        lax.fori_loop(lo, hi, run, 0)

    def inside(j):
        return (j >= 0) & (j < G)

    def enc_copy(j):
        part = pl.ds(pl.multiple_of(j * (E * C), E * C), E * C)
        return pltpu.make_async_copy(enc_hbm.at[:, part], enc.at[:, part], enc_sem.at[j])

    def near_copy(k):
        return pltpu.make_async_copy(near_hbm.at[k], near.at[k], near_sem.at[k])

    far_copy = pltpu.make_async_copy(far_hbm, far, far_sem)

    def z_copy(lane, j, to):
        return remote(z_out.at[lane, j], z_in.at[lane, j], z_s.at[lane], z_r.at[lane, j], b, to)

    def act_direct(k, j):
        return remote(acts.at[0, j], acts.at[k, j], ad_s.at[k], a_r.at[k - 1, j], b + k, w)

    def act_pass(k_from, k, j, to):
        return remote(acts.at[k_from, j], acts.at[k, j], af_s.at[k], a_r.at[k - 1, j], to, w)

    def share(k):
        return remote(p_out.at[k], p_in.at[k], p_s.at[k], p_r.at[k], b - k + B, w)

    def share_pair(k):
        return remote(p_out.at[k], p_in.at[k - 1], p_s.at[k], p_r.at[k - 1], b - 1, w)

    def share_wait(k):
        remote(p_out.at[k], p_in.at[k], p_s.at[k], p_r.at[k], b, w).wait_recv()

    def out_grad(k):
        return remote(og.at[0], og.at[k], o_s.at[k], o_r.at[k], b + k - B, w)

    def grad_pair(k):
        return remote(og.at[k], og.at[k + 1], o_s.at[k], o_r.at[k + 1], b + 1, w)

    def paired(k):
        return even if k % 2 == 0 else odd

    def duo_copy(k_from, k, j, to):
        return remote(terms.at[k_from, j], duo.at[k - 2, j], d_s.at[k_from], d_r.at[k - 2, j], to, w)

    def ret_copy(k_from, k, j, to):
        return remote(terms.at[k_from, j], ret.at[k, j], r_s.at[k_from], r_r.at[k - 1, j], to, w)

    def rel_copy(j):
        return remote(terms.at[2, j], rel.at[j], l_s, l_r.at[j], b + 2, w)

    def bias_copy(d):
        return remote(gb, gb, g_s.at[d], g_r, b, lax.rem(w + d, W))

    loop(0, G // E, lambda j: enc_copy(j).start())

    barrier = pltpu.get_barrier_semaphore()
    for d in range(1, W):
        pl.semaphore_signal(barrier, inc=1, device_id=(b, lax.rem(w + d, W)), device_id_type=pl.DeviceIdType.MESH)
    for d in range(1, B):
        pl.semaphore_signal(barrier, inc=1, device_id=(lax.rem(b + d, B), w), device_id_type=pl.DeviceIdType.MESH)

    fb, feats = blocks_ref.shape[0], bias_ref.shape[1]
    row_id = lax.broadcasted_iota(jnp.int32, (fb, feats), 0)
    lane_id = lax.broadcasted_iota(jnp.int32, (fb, feats), 1) // FBLK
    spread = jnp.where(row_id == lane_id, 1.0, 0.0).astype(BF)
    active = blocks_ref[...].astype(F32).astype(BF)
    mask[...] = lax.dot_general(active, spread, (((0,), (0,)), ((), ())), preferred_element_type=F32).astype(BF)
    recon_ref[...] = jnp.zeros(recon_ref.shape, F32)
    p_acc[...] = jnp.zeros(p_acc.shape, F32)
    pl.semaphore_wait(barrier, W + B - 2)

    def ends(phase, j):
        @pl.when(w == 0)
        def _():
            z_out[2 * phase, j] = own[j].astype(BF)
            z_copy(2 * phase, j, w + 1).start()

        @pl.when(w == W - 1)
        def _():
            z_out[2 * phase + 1, j] = own[j].astype(BF)
            z_copy(2 * phase + 1, j, w - 1).start()

    def first(j):
        @pl.when(lax.rem(j, E) == 0)
        def _():
            enc_copy(lax.div(j, E)).wait()

        own[j] = dot(x_ref[...], enc[:, col(j)])
        ends(0, j)

    loop(0, G, first)
    for k in range(N):
        near_copy(k).start()
    far_copy.start()

    def hop(phase, t):
        up = t - SKEW * (w - 1)
        down = t - SKEW * (W - 2 - w)

        @pl.when((w > 0) & inside(up))
        def _():
            z_copy(2 * phase, up, w).wait_recv()

            @pl.when(w < W - 1)
            def _():
                z_out[2 * phase, up] = (own[up] + z_in[2 * phase, up].astype(F32)).astype(BF)
                z_copy(2 * phase, up, w + 1).start()

        @pl.when((w < W - 1) & inside(down))
        def _():
            z_copy(2 * phase + 1, down, w).wait_recv()

            @pl.when(w > 0)
            def _():
                z_out[2 * phase + 1, down] = (own[down] + z_in[2 * phase + 1, down].astype(F32)).astype(BF)
                z_copy(2 * phase + 1, down, w - 1).start()

    def total(phase, j, put):
        @pl.when(w == 0)
        def _():
            put(own[j] + z_in[2 * phase + 1, j].astype(F32))

        @pl.when(w == W - 1)
        def _():
            put(own[j] + z_in[2 * phase, j].astype(F32))

        @pl.when((w > 0) & (w < W - 1))
        def _():
            put(own[j] + z_in[2 * phase, j].astype(F32) + z_in[2 * phase + 1, j].astype(F32))

    def act_sends(j, act):
        for k in range(2, N, 2):
            @pl.when((b + k < B) & not_mid)
            def _():
                act(act_direct(k, j))

        @pl.when(even)
        def _():
            act(act_pass(0, 1, j, b + 1))

        @pl.when(odd & (b + N - 1 < B) & not_mid)
        def _():
            act(act_direct(N - 1, j))

        @pl.when(mid | (even & (b + N < B) & (j >= H)))
        def _():
            act(act_direct(N, j))

    start = lambda c: c.start()

    def finish(j):
        def put(value):
            acts[0, j] = (mask[:, col(j)].astype(F32) * (value + bias_ref[:, col(j)])).astype(BF)

        total(0, j, put)
        act_sends(j, start)
        recon_ref[...] += dot(acts[0, j], near[0, col(j), :])
        for k in range(1, N):
            @pl.when(b < k)
            def _():
                p_acc[k] += dot(acts[0, j], near[k, col(j), :])

        @pl.when((b < N) & (j < H))
        def _():
            p_acc[N] += dot(acts[0, j], far[col(j), :])

    def inside_term(k, j):
        if k < N:
            recon_ref[...] += dot(acts[k, j], near[k, col(j), :])
        else:
            recon_ref[...] += dot(acts[k, j], far[col(j - H), :])

    def act_forwards(k, j, act):
        if k % 2 == 0 and k < N:
            @pl.when(even)
            def _():
                act(act_pass(k, k + 1, j, b + 1))

            @pl.when(odd)
            def _():
                act(act_pass(k, k - 1, j, b - 1))
        if k == N - 1:
            @pl.when(j >= H)
            def _():
                act(act_pass(k, N, j, b + 1))

    def arrival(k, j):
        return remote(acts.at[k, j], acts.at[k, j], ad_s.at[k], a_r.at[k - 1, j], b, w)

    def relay_sends(j, act):
        act(act_pass(N, 2, j, b - 2))

        @pl.when(odd)
        def _():
            act(act_pass(N, N - 1, j, b - 1))

    def inner(j):
        if relay:
            @pl.when(top)
            def _():
                arrival(N, j).wait_recv()
                relay_sends(j, start)

                @pl.when(j >= H)
                def _():
                    inside_term(N, j)
        for k in list(range(2, N, 2)) + [N - 1, N]:
            cond = b >= k
            if k >= N - 1:
                cond = cond & even & not_top
            if k == N:
                cond = cond & (j >= H)

            @pl.when(cond)
            def _():
                arrival(k, j).wait_recv()
                act_forwards(k, j, start)
                inside_term(k, j)

    def passed(j):
        for k in list(range(1, N, 2)) + [N]:
            cond = b >= k
            if k == N - 1:
                cond = cond & (odd | top)
            if k == N:
                cond = cond & odd & not_top
            if k == N:
                cond = cond & (j >= H)

            @pl.when(cond)
            def _():
                arrival(k, j).wait_recv()
                inside_term(k, j)


    def forward(t):
        hop(0, t)
        f = t - SKEW * (W - 2)

        @pl.when(f == 0)
        def _():
            for k in range(N):
                near_copy(k).wait()
            far_copy.wait()

        @pl.when(inside(f))
        def _():
            finish(f)

        for k in range(1, N + 1):
            if k > 1:
                @pl.when((f == G - 1) & (b < k) & odd)
                def _():
                    p_out[k] = p_acc[k].astype(BF)
                    share_pair(k).start()

            @pl.when((f == G + 1) & (b < k) & even)
            def _():
                if k < N:
                    share_wait(k)
                    p_acc[k] += p_in[k].astype(F32)
                p_out[k] = p_acc[k].astype(BF)
                share(k).start()

        i = f - AHEAD - late

        @pl.when(inside(i))
        def _():
            inner(i)

        p = i - BEHIND

        @pl.when(inside(p))
        def _():
            passed(p)

    loop(0, G + SKEW * (W - 2) + AHEAD + BEHIND + (LATE if relay else 0), forward)
    for k in range(1, N + 1):
        @pl.when((b + k >= B) & paired(k))
        def _():
            share_wait(k)
            recon_ref[...] += p_in[k].astype(F32)

    og[0] = (recon_ref[...] - tgt_ref[...].astype(F32)).astype(BF)
    for k in range(1, N + 1):
        @pl.when((b + k >= B) & paired(k))
        def _():
            out_grad(k).start()

    def back(j):
        for k in list(range(1, N, 2)) + [N] + list(range(2, N, 2)):
            cond = b >= k
            if k == N:
                cond = cond & (j >= H)

            @pl.when(cond)
            def _():
                rows = near[k, col(j), :] if k < N else far[col(j - H), :]
                terms[k, j] = dot_t(og[0], rows).astype(BF)
                duo_sends(k, j, start)

    def duo_sends(k, j, act):
        if k % 2 == 1 and k <= N - 3:
            @pl.when(even)
            def _():
                act(duo_copy(k, k + 1, j, b + 1))
        if k == 1:
            @pl.when(odd)
            def _():
                act(ret_copy(1, 1, j, b - 1))
        if k % 2 == 1 and k >= 3:
            @pl.when(odd)
            def _():
                act(duo_copy(k, k - 1, j, b - 1))
        if k == N - 1 and relay:
            @pl.when(even & top)
            def _():
                act(duo_copy(k, k, j, b + 1))
        if k == N:
            @pl.when(odd & not_top)
            def _():
                act(duo_copy(N, N - 1, j, b - 1))

            @pl.when(even & not_top)
            def _():
                act(ret_copy(N, N, j, b - N))

    def duo_wait(k, j):
        remote(duo.at[k - 2, j], duo.at[k - 2, j], d_s.at[k], d_r.at[k - 2, j], b, w).wait_recv()

    def duo_add(k, j):
        duo_wait(k, j)
        terms[k, j] = (terms[k, j].astype(F32) + duo[k - 2, j].astype(F32)).astype(BF)

    def down_sends(k, j, act):
        @pl.when(not_far_side)
        def _():
            act(ret_copy(k, k, j, b - k))
        if k == 2 and relay:
            @pl.when(far_side)
            def _():
                act(rel_copy(j))

    def down(j):
        for k in range(2, N, 2):
            @pl.when(b >= k)
            def _():
                duo_add(k, j)
                down_sends(k, j, start)

        @pl.when(even & (b >= N - 1) & not_top)
        def _():
            @pl.when(j >= H)
            def _():
                duo_add(N - 1, j)
            ret_copy(N - 1, N - 1, j, b - (N - 1)).start()

    def relay_down(j):
        remote(rel.at[j], rel.at[j], l_s, l_r.at[j], b, w).wait_recv()

        def put(value):
            @pl.when(j >= H)
            def _():
                terms[N, j] = (value + terms[N, j].astype(F32)).astype(BF)

            @pl.when(j < H)
            def _():
                terms[N, j] = value.astype(BF)

        @pl.when(even)
        def _():
            put(rel[j].astype(F32))

        @pl.when(odd)
        def _():
            duo_wait(N - 1, j)
            put(rel[j].astype(F32) + duo[N - 3, j].astype(F32))

        ret_copy(N, 2, j, b - N).start()

    def own_back(j):
        own[j] = dot_t(og[0], near[0, col(j), :])
        for k in range(1, N):
            @pl.when(b < k)
            def _():
                own[j] += dot_t(og[k], near[k, col(j), :])

        @pl.when((b < N) & (j < H))
        def _():
            own[j] += dot_t(og[N], far[col(j), :])

    def ret_add(k, j):
        remote(ret.at[k, j], ret.at[k, j], r_s.at[k], r_r.at[k - 1, j], b, w).wait_recv()
        own[j] += ret[k, j].astype(F32)

    def collect(j):
        @pl.when(even)
        def _():
            ret_add(1, j)
        for k in range(2, N, 2):
            @pl.when(b + k < B)
            def _():
                ret_add(k, j)

        @pl.when(odd & (b + N - 1 < B) & not_mid)
        def _():
            ret_add(N - 1, j)

        @pl.when(even & (b + N < B) & (j >= H) & not_mid)
        def _():
            ret_add(N, j)

    def finish_back(j):
        def put(value):
            grads = (mask[:, col(j)].astype(F32) * value).astype(BF)
            pg_ref[:, col(j)] = grads

            @pl.when(w == ROOT)
            def _():
                gb[:, col(j)] = jnp.sum(grads.astype(F32), axis=0, keepdims=True)

        total(1, j, put)


    def backward(t):
        @pl.when(t < G)
        def _():
            back(t)

        d = t - DUO

        @pl.when(inside(d))
        def _():
            down(d)

        if relay:
            r = t - RELAY

            @pl.when(top & inside(r))
            def _():
                relay_down(r)

        s = t - RING
        for k in range(1, N + 1):
            @pl.when((s == 0) & (b < k))
            def _():
                remote(og.at[k], og.at[k], o_s.at[k], o_r.at[k], b, w).wait_recv()
                if k < N:
                    @pl.when(even)
                    def _():
                        grad_pair(k).start()

        @pl.when(inside(s))
        def _():
            own_back(s)
            collect(s)
            ends(1, s)

        hop(1, s)
        f = s - SKEW * (W - 2)

        @pl.when(inside(f))
        def _():
            finish_back(f)

    loop(0, G + RING + SKEW * (W - 2), backward)

    @pl.when(w == ROOT)
    def _():
        for d in range(1, W):
            bias_copy(d).start()

    def sent(buf, k, n, sem, cond):
        @pl.when(cond)
        def _():
            part = buf.at[k, pl.ds(0, n)]
            remote(part, part, sem, sem, b, w).wait_send()

    for phase in range(2):
        sent(z_out, 2 * phase, G, z_s.at[2 * phase], w < W - 1)
        sent(z_out, 2 * phase + 1, G, z_s.at[2 * phase + 1], w > 0)
    sent(acts, 0, G, af_s.at[1], even)
    for k in range(2, N, 2):
        sent(acts, 0, G, ad_s.at[k], (b + k < B) & not_mid)
        sent(acts, k, G, af_s.at[k + 1], even & (b >= k))
        sent(acts, k, G, af_s.at[k - 1], odd & (b >= k))
    sent(acts, 0, G, ad_s.at[N - 1], odd & (b + N - 1 < B) & not_mid)
    sent(acts, 0, H, ad_s.at[N], even & (b + N < B) & not_mid)
    sent(acts, N - 1, H, af_s.at[N], even & (b >= N - 1) & not_top)
    for k in range(1, N, 2):
        if k <= N - 3:
            sent(terms, k, G, d_s.at[k], even & (b >= k))
        if k >= 3:
            sent(terms, k, G, d_s.at[k], odd & (b >= k))
    sent(terms, 1, G, r_s.at[1], odd)
    sent(terms, N, H, d_s.at[N], odd & (b >= N) & not_top)
    sent(terms, N, H, r_s.at[N], even & (b >= N) & not_top)
    for k in range(2, N, 2):
        sent(terms, k, G, r_s.at[k], (b >= k) & not_far_side if k == 2 else b >= k)
    sent(terms, N - 1, G, r_s.at[N - 1], even & (b >= N - 1) & not_top)
    if relay:
        sent(acts, 0, G, ad_s.at[N], mid)
        sent(acts, N, G, af_s.at[2], top)
        sent(acts, N, G, af_s.at[N - 1], top & odd)
        sent(terms, N - 1, G, d_s.at[N - 1], top & even)
        sent(terms, 2, G, l_s, far_side)
        sent(terms, N, G, r_s.at[N], top)
    for k in range(1, N + 1):
        @pl.when((b < k) & even)
        def _():
            share(k).wait_send()
            if k < N:
                grad_pair(k).wait_send()
        if k > 1:
            @pl.when((b < k) & odd)
            def _():
                share_pair(k).wait_send()

        @pl.when((b + k >= B) & paired(k))
        def _():
            out_grad(k).wait_send()

    @pl.when(w == ROOT)
    def _():
        for d in range(1, W):
            bias_copy(d).wait_send()

    @pl.when(w != ROOT)
    def _():
        bias_copy(1).wait_recv()

    gb_ref[...] = gb[...]


def weight_kernel(x_ref, pg_ref, recon_ref, gb_ref, grad_ref, recon_out, gb_out):
    grad_ref[...] = lax.dot_general(
        x_ref[...], pg_ref[...], (((0,), (0,)), ((), ())), preferred_element_type=F32
    ).astype(BF)
    recon_out[...] = recon_ref[...]
    gb_out[...] = gb_ref[...]


def on_device(B, W, inputs, encoder, enc_bias, active_blocks, near_decoders, far_decoders, targets):
    N = B // 2
    x = inputs[0]
    tok, width = x.shape
    feats = encoder.shape[2]
    half = far_decoders.shape[1]
    out_cols = targets.shape[2]
    C = min(half, 256)
    G = feats // C
    dma = pltpu.SemaphoreType.DMA
    blocks = lambda *lead: pltpu.VMEM((*lead, tok, C), BF)
    rows = lambda *lead: pltpu.VMEM((*lead, tok, out_cols), BF)
    vmem = pl.BlockSpec(memory_space=pltpu.VMEM)
    hbm = pl.BlockSpec(memory_space=pl.ANY)
    recon, pre_grad, bias_sum = pl.pallas_call(
        functools.partial(step_kernel, B, W, C, feats // active_blocks.shape[2]),
        out_shape=(jax.ShapeDtypeStruct((tok, out_cols), F32), jax.ShapeDtypeStruct((tok, feats), BF),
                   jax.ShapeDtypeStruct((1, feats), F32)),
        in_specs=[vmem, hbm, vmem, vmem, hbm, hbm, vmem],
        out_specs=(vmem, vmem, vmem),
        scratch_shapes=[
            pltpu.VMEM((width, feats), BF),
            pltpu.VMEM((N, feats, out_cols), BF),
            pltpu.VMEM((half, out_cols), BF),
            blocks(4, G), blocks(4, G), blocks(N + 1, G),
            pltpu.VMEM((N + 1, tok, out_cols), F32),
            rows(N + 1), rows(N + 1), rows(N + 1),
            blocks(N + 1, G), blocks(N - 2, G), blocks(N + 1, G), blocks(G),
            pltpu.VMEM((G, tok, C), F32),
            pltpu.VMEM((tok, feats), BF),
            pltpu.VMEM((1, feats), F32),
            dma((min(G, 4),)), dma((N,)), dma,
            dma((4,)), dma((4, G)),
            dma((N + 1,)), dma((N + 1,)), dma((N, G)),
            dma((N + 1,)), dma((N + 1,)), dma((N + 1,)), dma((N + 1,)),
            dma((N + 1,)), dma((N - 2, G)), dma((N + 1,)), dma((N, G)),
            dma, dma((G,)), dma((W,)), dma,
        ],
        compiler_params=pltpu.CompilerParams(
            collective_id=0, has_side_effects=True, vmem_limit_bytes=67_000_000),
        name="step",
    )(x, encoder[0], enc_bias, active_blocks[0].T, near_decoders[0], far_decoders[0], targets[0])
    steps = max(1, feats // 1024)
    tile = feats // steps
    part = tok // steps
    enc_grad, recon, bias_grad = pl.pallas_call(
        weight_kernel,
        grid=(steps,),
        out_shape=(jax.ShapeDtypeStruct((width, feats), BF), jax.ShapeDtypeStruct((tok, out_cols), F32),
                   jax.ShapeDtypeStruct((1, feats), F32)),
        in_specs=[pl.BlockSpec((tok, width), lambda i: (0, 0)), pl.BlockSpec((tok, tile), lambda i: (0, i)),
                  pl.BlockSpec((part, out_cols), lambda i: (i, 0)), pl.BlockSpec((1, tile), lambda i: (0, i))],
        out_specs=(pl.BlockSpec((width, tile), lambda i: (0, i)), pl.BlockSpec((part, out_cols), lambda i: (i, 0)),
                   pl.BlockSpec((1, tile), lambda i: (0, i))),
        name="weights",
    )(x, pre_grad, recon, bias_sum)
    return recon[None], enc_grad[None], bias_grad


def solution(mesh):
    return jax.shard_map(
        functools.partial(on_device, mesh.shape["blk"], mesh.shape["width"]),
        mesh=mesh,
        in_specs=(
            P("blk", None, "width"),
            P("blk", "width", None),
            P("blk", None),
            P("blk", None, None),
            P("blk", None, None, "width"),
            P("blk", None, "width"),
            P("blk", None, "width"),
        ),
        out_specs=(P("blk", None, "width"), P("blk", "width", None), P("blk", None)),
        check_vma=False,
    )
```

```python
import functools

import jax
import jax.numpy as jnp
from jax import lax
from jax.experimental import pallas as pl
from jax.experimental.pallas import tpu as pltpu
from jax.sharding import PartitionSpec as P

BF = jnp.bfloat16
F32 = jnp.float32


def dot(a, b):
    return jnp.dot(a, b, preferred_element_type=F32)


def dot_t(a, b):
    return lax.dot_general(a, b, (((1,), (1,)), ((), ())), preferred_element_type=F32)


def step_kernel(B, W, C, FBLK, x_ref, enc_hbm, bias_ref, blocks_ref, near_hbm, far_hbm, tgt_ref,
                recon_ref, pg_ref, gb_ref,
                enc, near, far, z_out, z_in, acts, p_acc, p_out, p_in, og, terms, duo, ret, rel, own, mask, gb,
                enc_sem, near_sem, far_sem, z_s, z_r, ad_s, af_s, a_r, p_s, p_r, o_s, o_r,
                d_s, d_r, r_s, r_r, l_s, l_r, g_s, g_r):
    N = B // 2
    G = own.shape[0]
    H = G // 2
    E = G // enc_sem.shape[0]
    ROOT = W // 2
    SKEW, AHEAD, LATE, EARLY, BEHIND = 4, 4, 2, 2, 4
    DUO, RELAY, RING = 2, 5, 8
    b = lax.axis_index("blk")
    w = lax.axis_index("width")
    even = lax.rem(b, 2) == 0
    odd = lax.rem(b, 2) == 1
    relay = N == 4
    mid = (b >= N - 2) & (b < N) & relay
    top = (b >= B - 2) & relay
    far_side = (b >= N) & (b < B - 2) & relay
    not_mid = jnp.logical_not(mid)
    not_top = jnp.logical_not(top)
    not_far_side = jnp.logical_not(far_side)
    chip = lax.div(b, 2)
    on_far_side = lax.div(chip, 2) - lax.div(chip, 3)
    on_top = lax.div(chip, 3)
    late = LATE * on_far_side - EARLY * on_top if relay else 0
    D = G // 4
    ring = RING - 2 * on_far_side - 4 * on_top if relay else RING
    upper = lax.div(2 * w, W)
    fill = SKEW * (upper * (w - 1) + (1 - upper) * (W - 2 - w))

    def col(j):
        return pl.ds(pl.multiple_of(j * C, C), C)

    def remote(src, dst, s, r, to_b, to_w):
        return pltpu.make_async_remote_copy(src_ref=src, dst_ref=dst, send_sem=s, recv_sem=r,
                                            device_id=(to_b, to_w), device_id_type=pl.DeviceIdType.MESH)

    def loop(lo, hi, body):
        def run(i, carry):
            body(i)
            return carry
        lax.fori_loop(lo, hi, run, 0)

    def inside(j):
        return (j >= 0) & (j < G)

    def enc_copy(j):
        part = pl.ds(pl.multiple_of(j * (E * C), E * C), E * C)
        return pltpu.make_async_copy(enc_hbm.at[:, part], enc.at[:, part], enc_sem.at[j])

    def near_copy(k):
        return pltpu.make_async_copy(near_hbm.at[k], near.at[k], near_sem.at[k])

    far_copy = pltpu.make_async_copy(far_hbm, far, far_sem)

    def z_copy(lane, j, to):
        return remote(z_out.at[lane, j], z_in.at[lane, j], z_s.at[lane], z_r.at[lane, j], b, to)

    def act_direct(k, j):
        return remote(acts.at[0, j], acts.at[k, j], ad_s.at[k], a_r.at[k - 1, j], b + k, w)

    def act_pass(k_from, k, j, to):
        return remote(acts.at[k_from, j], acts.at[k, j], af_s.at[k], a_r.at[k - 1, j], to, w)

    def share(k):
        return remote(p_out.at[k], p_in.at[k], p_s.at[k], p_r.at[k], b - k + B, w)

    def share_pair(k):
        return remote(p_out.at[k], p_in.at[k - 1], p_s.at[k], p_r.at[k - 1], b - 1, w)

    def share_wait(k):
        remote(p_out.at[k], p_in.at[k], p_s.at[k], p_r.at[k], b, w).wait_recv()

    def out_grad(k):
        return remote(og.at[0], og.at[k], o_s.at[k], o_r.at[k], b + k - B, w)

    def grad_pair(k):
        return remote(og.at[k], og.at[k + 1], o_s.at[k], o_r.at[k + 1], b + 1, w)

    def paired(k):
        return even if k % 2 == 0 else odd

    def duo_copy(k_from, k, j, to):
        return remote(terms.at[k_from, j], duo.at[k - 2, j], d_s.at[k_from], d_r.at[k - 2, j], to, w)

    def ret_copy(k_from, k, j, to):
        return remote(terms.at[k_from, j], ret.at[k, j], r_s.at[k_from], r_r.at[k - 1, j], to, w)

    def rel_copy(j):
        return remote(terms.at[2, j], rel.at[j], l_s, l_r.at[j], b + 2, w)

    def bias_copy(d):
        return remote(gb, gb, g_s.at[d], g_r, b, lax.rem(w + d, W))

    loop(0, G // E, lambda j: enc_copy(j).start())

    barrier = pltpu.get_barrier_semaphore()
    for d in range(1, W):
        pl.semaphore_signal(barrier, inc=1, device_id=(b, lax.rem(w + d, W)), device_id_type=pl.DeviceIdType.MESH)
    for d in range(1, B):
        pl.semaphore_signal(barrier, inc=1, device_id=(lax.rem(b + d, B), w), device_id_type=pl.DeviceIdType.MESH)

    fb, feats = blocks_ref.shape[0], bias_ref.shape[1]
    row_id = lax.broadcasted_iota(jnp.int32, (fb, feats), 0)
    lane_id = lax.broadcasted_iota(jnp.int32, (fb, feats), 1) // FBLK
    spread = jnp.where(row_id == lane_id, 1.0, 0.0).astype(BF)
    active = blocks_ref[...].astype(F32).astype(BF)
    mask[...] = lax.dot_general(active, spread, (((0,), (0,)), ((), ())), preferred_element_type=F32).astype(BF)
    recon_ref[...] = jnp.zeros(recon_ref.shape, F32)
    p_acc[...] = jnp.zeros(p_acc.shape, F32)
    pl.semaphore_wait(barrier, W + B - 2)

    def ends(phase, j):
        @pl.when(w == 0)
        def _():
            z_out[2 * phase, j] = own[j].astype(BF)
            z_copy(2 * phase, j, w + 1).start()

        @pl.when(w == W - 1)
        def _():
            z_out[2 * phase + 1, j] = own[j].astype(BF)
            z_copy(2 * phase + 1, j, w - 1).start()

    def first(j):
        @pl.when(lax.rem(j, E) == 0)
        def _():
            enc_copy(lax.div(j, E)).wait()

        own[j] = dot(x_ref[...], enc[:, col(j)])
        ends(0, j)

    loop(0, G, first)
    for k in range(N):
        near_copy(k).start()
    far_copy.start()

    def hop(phase, t):
        up = t - SKEW * (w - 1)
        down = t - SKEW * (W - 2 - w)

        @pl.when((w > 0) & inside(up))
        def _():
            z_copy(2 * phase, up, w).wait_recv()

            @pl.when(w < W - 1)
            def _():
                z_out[2 * phase, up] = (own[up] + z_in[2 * phase, up].astype(F32)).astype(BF)
                z_copy(2 * phase, up, w + 1).start()

        @pl.when((w < W - 1) & inside(down))
        def _():
            z_copy(2 * phase + 1, down, w).wait_recv()

            @pl.when(w > 0)
            def _():
                z_out[2 * phase + 1, down] = (own[down] + z_in[2 * phase + 1, down].astype(F32)).astype(BF)
                z_copy(2 * phase + 1, down, w - 1).start()

    def total(phase, j, put):
        @pl.when(w == 0)
        def _():
            put(own[j] + z_in[2 * phase + 1, j].astype(F32))

        @pl.when(w == W - 1)
        def _():
            put(own[j] + z_in[2 * phase, j].astype(F32))

        @pl.when((w > 0) & (w < W - 1))
        def _():
            put(own[j] + z_in[2 * phase, j].astype(F32) + z_in[2 * phase + 1, j].astype(F32))

    def act_sends(j, act):
        for k in range(2, N, 2):
            @pl.when((b + k < B) & (not_mid | (j < D)))
            def _():
                act(act_direct(k, j))

        @pl.when(even)
        def _():
            act(act_pass(0, 1, j, b + 1))

        @pl.when(odd & (b + N - 1 < B) & not_mid)
        def _():
            act(act_direct(N - 1, j))

        @pl.when(mid | (even & (b + N < B) & (j >= H)))
        def _():
            act(act_direct(N, j))

    start = lambda c: c.start()

    def finish(j):
        def put(value):
            acts[0, j] = (mask[:, col(j)].astype(F32) * (value + bias_ref[:, col(j)])).astype(BF)

        total(0, j, put)
        act_sends(j, start)
        recon_ref[...] += dot(acts[0, j], near[0, col(j), :])
        for k in range(1, N):
            @pl.when(b < k)
            def _():
                p_acc[k] += dot(acts[0, j], near[k, col(j), :])

        @pl.when((b < N) & (j < H))
        def _():
            p_acc[N] += dot(acts[0, j], far[col(j), :])

    def inside_term(k, j):
        if k < N:
            recon_ref[...] += dot(acts[k, j], near[k, col(j), :])
        else:
            recon_ref[...] += dot(acts[k, j], far[col(j - H), :])

    def act_forwards(k, j, act):
        if k % 2 == 0 and k < N:
            @pl.when(even)
            def _():
                act(act_pass(k, k + 1, j, b + 1))

            @pl.when(odd)
            def _():
                act(act_pass(k, k - 1, j, b - 1))
        if k == N - 1:
            @pl.when(j >= H)
            def _():
                act(act_pass(k, N, j, b + 1))

    def arrival(k, j):
        return remote(acts.at[k, j], acts.at[k, j], ad_s.at[k], a_r.at[k - 1, j], b, w)

    def relay_sends(j, act):
        @pl.when(j >= D)
        def _():
            act(act_pass(N, 2, j, b - 2))

        @pl.when(odd)
        def _():
            act(act_pass(N, N - 1, j, b - 1))

    def inner(j):
        if relay:
            @pl.when(top)
            def _():
                arrival(N, j).wait_recv()
                relay_sends(j, start)

                @pl.when(j >= H)
                def _():
                    inside_term(N, j)
        for k in list(range(2, N, 2)) + [N - 1, N]:
            cond = b >= k
            if k >= N - 1:
                cond = cond & even & not_top
            if k == N:
                cond = cond & (j >= H)

            @pl.when(cond)
            def _():
                arrival(k, j).wait_recv()
                act_forwards(k, j, start)
                inside_term(k, j)

    def passed(j):
        for k in list(range(1, N, 2)) + [N]:
            cond = b >= k
            if k == N - 1:
                cond = cond & (odd | top)
            if k == N:
                cond = cond & odd & not_top
            if k == N:
                cond = cond & (j >= H)

            @pl.when(cond)
            def _():
                arrival(k, j).wait_recv()
                inside_term(k, j)


    def forward(t):
        hop(0, t)
        f = t - fill

        @pl.when(f == 0)
        def _():
            for k in range(N):
                near_copy(k).wait()
            far_copy.wait()

        @pl.when(inside(f))
        def _():
            finish(f)

        for k in range(1, N + 1):
            if k > 1:
                @pl.when((f == G - 1) & (b < k) & odd)
                def _():
                    p_out[k] = p_acc[k].astype(BF)
                    share_pair(k).start()

            @pl.when((f == G + 1) & (b < k) & even)
            def _():
                if k < N:
                    share_wait(k)
                    p_acc[k] += p_in[k].astype(F32)
                p_out[k] = p_acc[k].astype(BF)
                share(k).start()

        i = f - AHEAD - late

        @pl.when(inside(i))
        def _():
            inner(i)

        p = i - BEHIND

        @pl.when(inside(p))
        def _():
            passed(p)

    loop(0, G + SKEW * (W - 2) + AHEAD + BEHIND + (LATE if relay else 0), forward)
    for k in range(1, N + 1):
        @pl.when((b + k >= B) & paired(k))
        def _():
            share_wait(k)
            recon_ref[...] += p_in[k].astype(F32)

    og[0] = (recon_ref[...] - tgt_ref[...].astype(F32)).astype(BF)
    for k in range(1, N + 1):
        @pl.when((b + k >= B) & paired(k))
        def _():
            out_grad(k).start()

    def back(j):
        for k in list(range(1, N, 2)) + [N] + list(range(2, N, 2)):
            cond = b >= k
            if k == N:
                cond = cond & (j >= H)

            @pl.when(cond)
            def _():
                rows = near[k, col(j), :] if k < N else far[col(j - H), :]
                terms[k, j] = dot_t(og[0], rows).astype(BF)
                duo_sends(k, j, start)

    def duo_sends(k, j, act):
        if k % 2 == 1 and k <= N - 3:
            @pl.when(even)
            def _():
                act(duo_copy(k, k + 1, j, b + 1))
        if k == 1:
            @pl.when(odd)
            def _():
                act(ret_copy(1, 1, j, b - 1))
        if k % 2 == 1 and k >= 3:
            @pl.when(odd)
            def _():
                act(duo_copy(k, k - 1, j, b - 1))
        if k == N - 1 and relay:
            @pl.when(even & top)
            def _():
                act(duo_copy(k, k, j, b + 1))
        if k == N:
            @pl.when(odd & not_top)
            def _():
                act(duo_copy(N, N - 1, j, b - 1))

            @pl.when(even & not_top)
            def _():
                act(ret_copy(N, N, j, b - N))

    def duo_wait(k, j):
        remote(duo.at[k - 2, j], duo.at[k - 2, j], d_s.at[k], d_r.at[k - 2, j], b, w).wait_recv()

    def duo_add(k, j):
        duo_wait(k, j)
        terms[k, j] = (terms[k, j].astype(F32) + duo[k - 2, j].astype(F32)).astype(BF)

    def down_sends(k, j, act):
        @pl.when(not_far_side)
        def _():
            act(ret_copy(k, k, j, b - k))
        if k == 2 and relay:
            @pl.when(far_side)
            def _():
                act(rel_copy(j))

    def down(j):
        for k in range(2, N, 2):
            @pl.when(b >= k)
            def _():
                duo_add(k, j)
                down_sends(k, j, start)

        @pl.when(even & (b >= N - 1) & not_top)
        def _():
            @pl.when(j >= H)
            def _():
                duo_add(N - 1, j)
            ret_copy(N - 1, N - 1, j, b - (N - 1)).start()

    def relay_down(j):
        remote(rel.at[j], rel.at[j], l_s, l_r.at[j], b, w).wait_recv()

        def put(value):
            @pl.when(j >= H)
            def _():
                terms[N, j] = (value + terms[N, j].astype(F32)).astype(BF)

            @pl.when(j < H)
            def _():
                terms[N, j] = value.astype(BF)

        @pl.when(even)
        def _():
            put(rel[j].astype(F32))

        @pl.when(odd)
        def _():
            duo_wait(N - 1, j)
            put(rel[j].astype(F32) + duo[N - 3, j].astype(F32))

        ret_copy(N, 2, j, b - N).start()

    def own_back(j):
        own[j] = dot_t(og[0], near[0, col(j), :])
        for k in range(1, N):
            @pl.when(b < k)
            def _():
                own[j] += dot_t(og[k], near[k, col(j), :])

        @pl.when((b < N) & (j < H))
        def _():
            own[j] += dot_t(og[N], far[col(j), :])

    def ret_add(k, j):
        remote(ret.at[k, j], ret.at[k, j], r_s.at[k], r_r.at[k - 1, j], b, w).wait_recv()
        own[j] += ret[k, j].astype(F32)

    def collect(j):
        @pl.when(even)
        def _():
            ret_add(1, j)
        for k in range(2, N, 2):
            @pl.when(b + k < B)
            def _():
                ret_add(k, j)

        @pl.when(odd & (b + N - 1 < B) & not_mid)
        def _():
            ret_add(N - 1, j)

        @pl.when(even & (b + N < B) & (j >= H) & not_mid)
        def _():
            ret_add(N, j)

    def finish_back(j):
        def put(value):
            grads = (mask[:, col(j)].astype(F32) * value).astype(BF)
            pg_ref[:, col(j)] = grads

            @pl.when(w == ROOT)
            def _():
                gb[:, col(j)] = jnp.sum(grads.astype(F32), axis=0, keepdims=True)

        total(1, j, put)


    def backward(t):
        @pl.when(t < G)
        def _():
            back(t)

        d = t - DUO

        @pl.when(inside(d))
        def _():
            down(d)

        if relay:
            r = t - RELAY

            @pl.when(top & inside(r))
            def _():
                relay_down(r)

        s = t - ring
        for k in range(1, N + 1):
            @pl.when((s == 0) & (b < k))
            def _():
                remote(og.at[k], og.at[k], o_s.at[k], o_r.at[k], b, w).wait_recv()
                if k < N:
                    @pl.when(even)
                    def _():
                        grad_pair(k).start()

        @pl.when(inside(s))
        def _():
            own_back(s)
            collect(s)
            ends(1, s)

        hop(1, s)
        f = s - SKEW * (W - 2)

        @pl.when(inside(f))
        def _():
            finish_back(f)

    loop(0, G + RING + SKEW * (W - 2), backward)

    @pl.when(w == ROOT)
    def _():
        for d in range(1, W):
            bias_copy(d).start()

    def sent(buf, k, n, sem, cond):
        @pl.when(cond)
        def _():
            part = buf.at[k, pl.ds(0, n)]
            remote(part, part, sem, sem, b, w).wait_send()

    for phase in range(2):
        sent(z_out, 2 * phase, G, z_s.at[2 * phase], w < W - 1)
        sent(z_out, 2 * phase + 1, G, z_s.at[2 * phase + 1], w > 0)
    sent(acts, 0, G, af_s.at[1], even)
    for k in range(2, N, 2):
        sent(acts, 0, G, ad_s.at[k], (b + k < B) & not_mid)
        sent(acts, k, G, af_s.at[k + 1], even & (b >= k))
        sent(acts, k, G, af_s.at[k - 1], odd & (b >= k))
    sent(acts, 0, G, ad_s.at[N - 1], odd & (b + N - 1 < B) & not_mid)
    sent(acts, 0, H, ad_s.at[N], even & (b + N < B) & not_mid)
    sent(acts, N - 1, H, af_s.at[N], even & (b >= N - 1) & not_top)
    for k in range(1, N, 2):
        if k <= N - 3:
            sent(terms, k, G, d_s.at[k], even & (b >= k))
        if k >= 3:
            sent(terms, k, G, d_s.at[k], odd & (b >= k))
    sent(terms, 1, G, r_s.at[1], odd)
    sent(terms, N, H, d_s.at[N], odd & (b >= N) & not_top)
    sent(terms, N, H, r_s.at[N], even & (b >= N) & not_top)
    for k in range(2, N, 2):
        sent(terms, k, G, r_s.at[k], (b >= k) & not_far_side if k == 2 else b >= k)
    sent(terms, N - 1, G, r_s.at[N - 1], even & (b >= N - 1) & not_top)
    if relay:
        sent(acts, 0, G, ad_s.at[N], mid)
        sent(acts, 0, D, ad_s.at[2], mid)
        sent(acts, N, G - D, af_s.at[2], top)
        sent(acts, N, G, af_s.at[N - 1], top & odd)
        sent(terms, N - 1, G, d_s.at[N - 1], top & even)
        sent(terms, 2, G, l_s, far_side)
        sent(terms, N, G, r_s.at[N], top)
    for k in range(1, N + 1):
        @pl.when((b < k) & even)
        def _():
            share(k).wait_send()
            if k < N:
                grad_pair(k).wait_send()
        if k > 1:
            @pl.when((b < k) & odd)
            def _():
                share_pair(k).wait_send()

        @pl.when((b + k >= B) & paired(k))
        def _():
            out_grad(k).wait_send()

    @pl.when(w == ROOT)
    def _():
        for d in range(1, W):
            bias_copy(d).wait_send()

    @pl.when(w != ROOT)
    def _():
        bias_copy(1).wait_recv()

    gb_ref[...] = gb[...]


def weight_kernel(x_ref, pg_ref, recon_ref, gb_ref, grad_ref, recon_out, gb_out):
    grad_ref[...] = lax.dot_general(
        x_ref[...], pg_ref[...], (((0,), (0,)), ((), ())), preferred_element_type=F32
    ).astype(BF)
    recon_out[...] = recon_ref[...]
    gb_out[...] = gb_ref[...]


def on_device(B, W, inputs, encoder, enc_bias, active_blocks, near_decoders, far_decoders, targets):
    N = B // 2
    x = inputs[0]
    tok, width = x.shape
    feats = encoder.shape[2]
    half = far_decoders.shape[1]
    out_cols = targets.shape[2]
    C = min(half, 256)
    G = feats // C
    dma = pltpu.SemaphoreType.DMA
    blocks = lambda *lead: pltpu.VMEM((*lead, tok, C), BF)
    rows = lambda *lead: pltpu.VMEM((*lead, tok, out_cols), BF)
    vmem = pl.BlockSpec(memory_space=pltpu.VMEM)
    hbm = pl.BlockSpec(memory_space=pl.ANY)
    recon, pre_grad, bias_sum = pl.pallas_call(
        functools.partial(step_kernel, B, W, C, feats // active_blocks.shape[2]),
        out_shape=(jax.ShapeDtypeStruct((tok, out_cols), F32), jax.ShapeDtypeStruct((tok, feats), BF),
                   jax.ShapeDtypeStruct((1, feats), F32)),
        in_specs=[vmem, hbm, vmem, vmem, hbm, hbm, vmem],
        out_specs=(vmem, vmem, vmem),
        scratch_shapes=[
            pltpu.VMEM((width, feats), BF),
            pltpu.VMEM((N, feats, out_cols), BF),
            pltpu.VMEM((half, out_cols), BF),
            blocks(4, G), blocks(4, G), blocks(N + 1, G),
            pltpu.VMEM((N + 1, tok, out_cols), F32),
            rows(N + 1), rows(N + 1), rows(N + 1),
            blocks(N + 1, G), blocks(N - 2, G), blocks(N + 1, G), blocks(G),
            pltpu.VMEM((G, tok, C), F32),
            pltpu.VMEM((tok, feats), BF),
            pltpu.VMEM((1, feats), F32),
            dma((min(G, 4),)), dma((N,)), dma,
            dma((4,)), dma((4, G)),
            dma((N + 1,)), dma((N + 1,)), dma((N, G)),
            dma((N + 1,)), dma((N + 1,)), dma((N + 1,)), dma((N + 1,)),
            dma((N + 1,)), dma((N - 2, G)), dma((N + 1,)), dma((N, G)),
            dma, dma((G,)), dma((W,)), dma,
        ],
        compiler_params=pltpu.CompilerParams(
            collective_id=0, has_side_effects=True, vmem_limit_bytes=67_000_000),
        name="step",
    )(x, encoder[0], enc_bias, active_blocks[0].T, near_decoders[0], far_decoders[0], targets[0])
    steps = max(1, feats // 2048)
    tile = feats // steps
    part = tok // steps
    enc_grad, recon, bias_grad = pl.pallas_call(
        weight_kernel,
        grid=(steps,),
        out_shape=(jax.ShapeDtypeStruct((width, feats), BF), jax.ShapeDtypeStruct((tok, out_cols), F32),
                   jax.ShapeDtypeStruct((1, feats), F32)),
        in_specs=[pl.BlockSpec((tok, width), lambda i: (0, 0)), pl.BlockSpec((tok, tile), lambda i: (0, i)),
                  pl.BlockSpec((part, out_cols), lambda i: (i, 0)), pl.BlockSpec((1, tile), lambda i: (0, i))],
        out_specs=(pl.BlockSpec((width, tile), lambda i: (0, i)), pl.BlockSpec((part, out_cols), lambda i: (i, 0)),
                   pl.BlockSpec((1, tile), lambda i: (0, i))),
        name="weights",
    )(x, pre_grad, recon, bias_sum)
    return recon[None], enc_grad[None], bias_grad


def solution(mesh):
    return jax.shard_map(
        functools.partial(on_device, mesh.shape["blk"], mesh.shape["width"]),
        mesh=mesh,
        in_specs=(
            P("blk", None, "width"),
            P("blk", "width", None),
            P("blk", None),
            P("blk", None, None),
            P("blk", None, None, "width"),
            P("blk", None, "width"),
            P("blk", None, "width"),
        ),
        out_specs=(P("blk", None, "width"), P("blk", "width", None), P("blk", None)),
        check_vma=False,
    )
```

```python
import functools

import jax
import jax.numpy as jnp
from jax import lax
from jax.experimental import pallas as pl
from jax.experimental.pallas import tpu as pltpu
from jax.sharding import PartitionSpec as P

BF = jnp.bfloat16
F32 = jnp.float32


def dot(a, b):
    return jnp.dot(a, b, preferred_element_type=F32)


def dot_t(a, b):
    return lax.dot_general(a, b, (((1,), (1,)), ((), ())), preferred_element_type=F32)


def step_kernel(B, W, C, FBLK, x_hbm, enc_hbm, bias_hbm, blocks_hbm, near_hbm, far_hbm, tgt_hbm,
                recon_ref, pg_ref, gb_ref,
                x_ref, bias_ref, blocks_ref, tgt_ref, enc, near, far, z_out, z_in, acts, p_acc, p_out, p_in, og, terms, duo, ret, rel, own, mask, gb,
                in_sem, enc_sem, near_sem, far_sem, z_s, z_r, ad_s, af_s, a_r, p_s, p_r, o_s, o_r,
                d_s, d_r, r_s, r_r, l_s, l_r, g_s, g_r):
    N = B // 2
    G = own.shape[0]
    H = G // 2
    E = G // enc_sem.shape[0]
    ROOT = W // 2
    SKEW, AHEAD, LATE, EARLY, BEHIND = 4, 4, 2, 2, 2
    DUO, RELAY, RING = 2, 5, 8
    b = lax.axis_index("blk")
    w = lax.axis_index("width")
    even = lax.rem(b, 2) == 0
    odd = lax.rem(b, 2) == 1
    relay = N == 4
    mid = (b >= N - 2) & (b < N) & relay
    top = (b >= B - 2) & relay
    far_side = (b >= N) & (b < B - 2) & relay
    not_mid = jnp.logical_not(mid)
    not_top = jnp.logical_not(top)
    not_far_side = jnp.logical_not(far_side)
    chip = lax.div(b, 2)
    on_far_side = lax.div(chip, 2) - lax.div(chip, 3)
    on_top = lax.div(chip, 3)
    late = LATE * on_far_side - EARLY * on_top if relay else 0
    D = G // 4
    ring = RING - 2 * on_far_side - 4 * on_top if relay else RING
    upper = lax.div(2 * w, W)
    fill = SKEW * (upper * (w - 1) + (1 - upper) * (W - 2 - w))

    def col(j):
        return pl.ds(pl.multiple_of(j * C, C), C)

    def remote(src, dst, s, r, to_b, to_w):
        return pltpu.make_async_remote_copy(src_ref=src, dst_ref=dst, send_sem=s, recv_sem=r,
                                            device_id=(to_b, to_w), device_id_type=pl.DeviceIdType.MESH)

    def loop(lo, hi, body):
        def run(i, carry):
            body(i)
            return carry
        lax.fori_loop(lo, hi, run, 0)

    def inside(j):
        return (j >= 0) & (j < G)

    def enc_copy(j):
        part = pl.ds(pl.multiple_of(j * (E * C), E * C), E * C)
        return pltpu.make_async_copy(enc_hbm.at[:, part], enc.at[:, part], enc_sem.at[j])

    def near_copy(k):
        return pltpu.make_async_copy(near_hbm.at[k], near.at[k], near_sem.at[k])

    far_copy = pltpu.make_async_copy(far_hbm, far, far_sem)
    pairs = ((blocks_hbm, blocks_ref), (x_hbm, x_ref), (bias_hbm, bias_ref), (tgt_hbm, tgt_ref))
    loads = [pltpu.make_async_copy(src, dst, in_sem.at[i]) for i, (src, dst) in enumerate(pairs)]

    def z_copy(lane, j, to):
        return remote(z_out.at[lane, j], z_in.at[lane, j], z_s.at[lane], z_r.at[lane, j], b, to)

    def act_direct(k, j):
        return remote(acts.at[0, j], acts.at[k, j], ad_s.at[k], a_r.at[k - 1, j], b + k, w)

    def act_pass(k_from, k, j, to):
        return remote(acts.at[k_from, j], acts.at[k, j], af_s.at[k], a_r.at[k - 1, j], to, w)

    def share(k):
        return remote(p_out.at[k], p_in.at[k], p_s.at[k], p_r.at[k], b - k + B, w)

    def share_pair(k):
        return remote(p_out.at[k], p_in.at[k - 1], p_s.at[k], p_r.at[k - 1], b - 1, w)

    def share_wait(k):
        remote(p_out.at[k], p_in.at[k], p_s.at[k], p_r.at[k], b, w).wait_recv()

    def out_grad(k):
        return remote(og.at[0], og.at[k], o_s.at[k], o_r.at[k], b + k - B, w)

    def grad_pair(k):
        return remote(og.at[k], og.at[k + 1], o_s.at[k], o_r.at[k + 1], b + 1, w)

    def paired(k):
        return even if k % 2 == 0 else odd

    def duo_copy(k_from, k, j, to):
        return remote(terms.at[k_from, j], duo.at[k - 2, j], d_s.at[k_from], d_r.at[k - 2, j], to, w)

    def ret_copy(k_from, k, j, to):
        return remote(terms.at[k_from, j], ret.at[k, j], r_s.at[k_from], r_r.at[k - 1, j], to, w)

    def rel_copy(j):
        return remote(terms.at[2, j], rel.at[j], l_s, l_r.at[j], b + 2, w)

    def bias_copy(d):
        return remote(gb, gb, g_s.at[d], g_r, b, lax.rem(w + d, W))

    barrier = pltpu.get_barrier_semaphore()
    for d in range(1, W):
        pl.semaphore_signal(barrier, inc=1, device_id=(b, lax.rem(w + d, W)), device_id_type=pl.DeviceIdType.MESH)
    for d in range(1, B):
        pl.semaphore_signal(barrier, inc=1, device_id=(lax.rem(b + d, B), w), device_id_type=pl.DeviceIdType.MESH)

    for load in loads:
        load.start()
    loop(0, G // E, lambda j: enc_copy(j).start())
    fb, feats = blocks_ref.shape[0], bias_ref.shape[1]
    row_id = lax.broadcasted_iota(jnp.int32, (fb, feats), 0)
    lane_id = lax.broadcasted_iota(jnp.int32, (fb, feats), 1) // FBLK
    spread = jnp.where(row_id == lane_id, 1.0, 0.0).astype(BF)
    loads[0].wait()
    active = blocks_ref[...].astype(F32).astype(BF)
    mask[...] = lax.dot_general(active, spread, (((0,), (0,)), ((), ())), preferred_element_type=F32).astype(BF)
    recon_ref[...] = jnp.zeros(recon_ref.shape, F32)
    p_acc[...] = jnp.zeros(p_acc.shape, F32)
    for load in loads[1:]:
        load.wait()
    pl.semaphore_wait(barrier, W + B - 2)

    def ends(phase, j):
        @pl.when(w == 0)
        def _():
            z_out[2 * phase, j] = own[j].astype(BF)
            z_copy(2 * phase, j, w + 1).start()

        @pl.when(w == W - 1)
        def _():
            z_out[2 * phase + 1, j] = own[j].astype(BF)
            z_copy(2 * phase + 1, j, w - 1).start()

    def first(j):
        @pl.when(lax.rem(j, E) == 0)
        def _():
            enc_copy(lax.div(j, E)).wait()

        own[j] = dot(x_ref[...], enc[:, col(j)])
        ends(0, j)

    loop(0, G, first)
    for k in range(N):
        near_copy(k).start()
    far_copy.start()

    def hop(phase, t):
        up = t - SKEW * (w - 1)
        down = t - SKEW * (W - 2 - w)

        @pl.when((w > 0) & inside(up))
        def _():
            z_copy(2 * phase, up, w).wait_recv()

            @pl.when(w < W - 1)
            def _():
                z_out[2 * phase, up] = (own[up] + z_in[2 * phase, up].astype(F32)).astype(BF)
                z_copy(2 * phase, up, w + 1).start()

        @pl.when((w < W - 1) & inside(down))
        def _():
            z_copy(2 * phase + 1, down, w).wait_recv()

            @pl.when(w > 0)
            def _():
                z_out[2 * phase + 1, down] = (own[down] + z_in[2 * phase + 1, down].astype(F32)).astype(BF)
                z_copy(2 * phase + 1, down, w - 1).start()

    def total(phase, j, put):
        @pl.when(w == 0)
        def _():
            put(own[j] + z_in[2 * phase + 1, j].astype(F32))

        @pl.when(w == W - 1)
        def _():
            put(own[j] + z_in[2 * phase, j].astype(F32))

        @pl.when((w > 0) & (w < W - 1))
        def _():
            put(own[j] + z_in[2 * phase, j].astype(F32) + z_in[2 * phase + 1, j].astype(F32))

    def act_sends(j, act):
        for k in range(2, N, 2):
            @pl.when((b + k < B) & (not_mid | (j < D)))
            def _():
                act(act_direct(k, j))

        @pl.when(even)
        def _():
            act(act_pass(0, 1, j, b + 1))

        @pl.when(odd & (b + N - 1 < B) & not_mid)
        def _():
            act(act_direct(N - 1, j))

        @pl.when(mid | (even & (b + N < B) & (j >= H)))
        def _():
            act(act_direct(N, j))

    start = lambda c: c.start()

    def finish(j):
        def put(value):
            acts[0, j] = (mask[:, col(j)].astype(F32) * (value + bias_ref[:, col(j)])).astype(BF)

        total(0, j, put)
        act_sends(j, start)
        recon_ref[...] += dot(acts[0, j], near[0, col(j), :])
        for k in range(1, N):
            @pl.when(b < k)
            def _():
                p_acc[k] += dot(acts[0, j], near[k, col(j), :])

        @pl.when((b < N) & (j < H))
        def _():
            p_acc[N] += dot(acts[0, j], far[col(j), :])

    def inside_term(k, j):
        if k < N:
            recon_ref[...] += dot(acts[k, j], near[k, col(j), :])
        else:
            recon_ref[...] += dot(acts[k, j], far[col(j - H), :])

    def act_forwards(k, j, act):
        if k % 2 == 0 and k < N:
            @pl.when(even)
            def _():
                act(act_pass(k, k + 1, j, b + 1))

            @pl.when(odd)
            def _():
                act(act_pass(k, k - 1, j, b - 1))
        if k == N - 1:
            @pl.when(j >= H)
            def _():
                act(act_pass(k, N, j, b + 1))

    def arrival(k, j):
        return remote(acts.at[k, j], acts.at[k, j], ad_s.at[k], a_r.at[k - 1, j], b, w)

    def relay_sends(j, act):
        @pl.when(j >= D)
        def _():
            act(act_pass(N, 2, j, b - 2))

        @pl.when(odd)
        def _():
            act(act_pass(N, N - 1, j, b - 1))

    def inner(j):
        if relay:
            @pl.when(top)
            def _():
                arrival(N, j).wait_recv()
                relay_sends(j, start)

                @pl.when(j >= H)
                def _():
                    inside_term(N, j)
        for k in list(range(2, N, 2)) + [N - 1, N]:
            cond = b >= k
            if k >= N - 1:
                cond = cond & even & not_top
            if k == N:
                cond = cond & (j >= H)

            @pl.when(cond)
            def _():
                arrival(k, j).wait_recv()
                act_forwards(k, j, start)
                inside_term(k, j)

    def passed(j):
        for k in list(range(1, N, 2)) + [N]:
            cond = b >= k
            if k == N - 1:
                cond = cond & (odd | top)
            if k == N:
                cond = cond & odd & not_top
            if k == N:
                cond = cond & (j >= H)

            @pl.when(cond)
            def _():
                arrival(k, j).wait_recv()
                inside_term(k, j)


    def forward(t):
        hop(0, t)
        f = t - fill

        @pl.when(f == 0)
        def _():
            for k in range(N):
                near_copy(k).wait()
            far_copy.wait()

        @pl.when(inside(f))
        def _():
            finish(f)

        for k in range(1, N + 1):
            if k > 1:
                @pl.when((f == G - 1) & (b < k) & odd)
                def _():
                    p_out[k] = p_acc[k].astype(BF)
                    share_pair(k).start()

            @pl.when((f == G + 1) & (b < k) & even)
            def _():
                if k < N:
                    share_wait(k)
                    p_acc[k] += p_in[k].astype(F32)
                p_out[k] = p_acc[k].astype(BF)
                share(k).start()

        i = f - AHEAD - late

        @pl.when(inside(i))
        def _():
            inner(i)

        p = i - BEHIND

        @pl.when(inside(p))
        def _():
            passed(p)

    loop(0, G + SKEW * (W - 2) + AHEAD + BEHIND + (LATE if relay else 0), forward)
    for k in range(1, N + 1):
        @pl.when((b + k >= B) & paired(k))
        def _():
            share_wait(k)
            recon_ref[...] += p_in[k].astype(F32)

    og[0] = (recon_ref[...] - tgt_ref[...].astype(F32)).astype(BF)
    for k in range(1, N + 1):
        @pl.when((b + k >= B) & paired(k))
        def _():
            out_grad(k).start()

    def back(j):
        for k in list(range(1, N, 2)) + [N] + list(range(2, N, 2)):
            cond = b >= k
            if k == N:
                cond = cond & (j >= H)

            @pl.when(cond)
            def _():
                rows = near[k, col(j), :] if k < N else far[col(j - H), :]
                terms[k, j] = dot_t(og[0], rows).astype(BF)
                duo_sends(k, j, start)

    def duo_sends(k, j, act):
        if k % 2 == 1 and k <= N - 3:
            @pl.when(even)
            def _():
                act(duo_copy(k, k + 1, j, b + 1))
        if k == 1:
            @pl.when(odd)
            def _():
                act(ret_copy(1, 1, j, b - 1))
        if k % 2 == 1 and k >= 3:
            @pl.when(odd)
            def _():
                act(duo_copy(k, k - 1, j, b - 1))
        if k == N - 1 and relay:
            @pl.when(even & top)
            def _():
                act(duo_copy(k, k, j, b + 1))
        if k == N:
            @pl.when(odd & not_top)
            def _():
                act(duo_copy(N, N - 1, j, b - 1))

            @pl.when(even & not_top)
            def _():
                act(ret_copy(N, N, j, b - N))

    def duo_wait(k, j):
        remote(duo.at[k - 2, j], duo.at[k - 2, j], d_s.at[k], d_r.at[k - 2, j], b, w).wait_recv()

    def duo_add(k, j):
        duo_wait(k, j)
        terms[k, j] = (terms[k, j].astype(F32) + duo[k - 2, j].astype(F32)).astype(BF)

    def down_sends(k, j, act):
        @pl.when(not_far_side)
        def _():
            act(ret_copy(k, k, j, b - k))
        if k == 2 and relay:
            @pl.when(far_side)
            def _():
                act(rel_copy(j))

    def down(j):
        for k in range(2, N, 2):
            @pl.when(b >= k)
            def _():
                duo_add(k, j)
                down_sends(k, j, start)

        @pl.when(even & (b >= N - 1) & not_top)
        def _():
            @pl.when(j >= H)
            def _():
                duo_add(N - 1, j)
            ret_copy(N - 1, N - 1, j, b - (N - 1)).start()

    def relay_down(j):
        remote(rel.at[j], rel.at[j], l_s, l_r.at[j], b, w).wait_recv()

        def put(value):
            @pl.when(j >= H)
            def _():
                terms[N, j] = (value + terms[N, j].astype(F32)).astype(BF)

            @pl.when(j < H)
            def _():
                terms[N, j] = value.astype(BF)

        @pl.when(even)
        def _():
            put(rel[j].astype(F32))

        @pl.when(odd)
        def _():
            duo_wait(N - 1, j)
            put(rel[j].astype(F32) + duo[N - 3, j].astype(F32))

        ret_copy(N, 2, j, b - N).start()

    def own_back(j):
        own[j] = dot_t(og[0], near[0, col(j), :])
        for k in range(1, N):
            @pl.when(b < k)
            def _():
                own[j] += dot_t(og[k], near[k, col(j), :])

        @pl.when((b < N) & (j < H))
        def _():
            own[j] += dot_t(og[N], far[col(j), :])

    def ret_add(k, j):
        remote(ret.at[k, j], ret.at[k, j], r_s.at[k], r_r.at[k - 1, j], b, w).wait_recv()
        own[j] += ret[k, j].astype(F32)

    def collect(j):
        @pl.when(even)
        def _():
            ret_add(1, j)
        for k in range(2, N, 2):
            @pl.when(b + k < B)
            def _():
                ret_add(k, j)

        @pl.when(odd & (b + N - 1 < B) & not_mid)
        def _():
            ret_add(N - 1, j)

        @pl.when(even & (b + N < B) & (j >= H) & not_mid)
        def _():
            ret_add(N, j)

    def finish_back(j):
        def put(value):
            grads = (mask[:, col(j)].astype(F32) * value).astype(BF)
            pg_ref[:, col(j)] = grads

            @pl.when(w == ROOT)
            def _():
                gb[:, col(j)] = jnp.sum(grads.astype(F32), axis=0, keepdims=True)

        total(1, j, put)


    def backward(t):
        @pl.when(t < G)
        def _():
            back(t)

        d = t - DUO

        @pl.when(inside(d))
        def _():
            down(d)

        if relay:
            r = t - RELAY

            @pl.when(top & inside(r))
            def _():
                relay_down(r)

        s = t - ring
        for k in range(1, N + 1):
            @pl.when((s == 0) & (b < k))
            def _():
                remote(og.at[k], og.at[k], o_s.at[k], o_r.at[k], b, w).wait_recv()
                if k < N:
                    @pl.when(even)
                    def _():
                        grad_pair(k).start()

        @pl.when(inside(s))
        def _():
            own_back(s)
            collect(s)
            ends(1, s)

        hop(1, s)
        f = s - SKEW * (W - 2)

        @pl.when(inside(f))
        def _():
            finish_back(f)

    loop(0, G + RING + SKEW * (W - 2), backward)

    @pl.when(w == ROOT)
    def _():
        for d in range(1, W):
            bias_copy(d).start()

    def sent(buf, k, n, sem, cond):
        @pl.when(cond)
        def _():
            part = buf.at[k, pl.ds(0, n)]
            remote(part, part, sem, sem, b, w).wait_send()

    for phase in range(2):
        sent(z_out, 2 * phase, G, z_s.at[2 * phase], w < W - 1)
        sent(z_out, 2 * phase + 1, G, z_s.at[2 * phase + 1], w > 0)
    sent(acts, 0, G, af_s.at[1], even)
    for k in range(2, N, 2):
        sent(acts, 0, G, ad_s.at[k], (b + k < B) & not_mid)
        sent(acts, k, G, af_s.at[k + 1], even & (b >= k))
        sent(acts, k, G, af_s.at[k - 1], odd & (b >= k))
    sent(acts, 0, G, ad_s.at[N - 1], odd & (b + N - 1 < B) & not_mid)
    sent(acts, 0, H, ad_s.at[N], even & (b + N < B) & not_mid)
    sent(acts, N - 1, H, af_s.at[N], even & (b >= N - 1) & not_top)
    for k in range(1, N, 2):
        if k <= N - 3:
            sent(terms, k, G, d_s.at[k], even & (b >= k))
        if k >= 3:
            sent(terms, k, G, d_s.at[k], odd & (b >= k))
    sent(terms, 1, G, r_s.at[1], odd)
    sent(terms, N, H, d_s.at[N], odd & (b >= N) & not_top)
    sent(terms, N, H, r_s.at[N], even & (b >= N) & not_top)
    for k in range(2, N, 2):
        sent(terms, k, G, r_s.at[k], (b >= k) & not_far_side if k == 2 else b >= k)
    sent(terms, N - 1, G, r_s.at[N - 1], even & (b >= N - 1) & not_top)
    if relay:
        sent(acts, 0, G, ad_s.at[N], mid)
        sent(acts, 0, D, ad_s.at[2], mid)
        sent(acts, N, G - D, af_s.at[2], top)
        sent(acts, N, G, af_s.at[N - 1], top & odd)
        sent(terms, N - 1, G, d_s.at[N - 1], top & even)
        sent(terms, 2, G, l_s, far_side)
        sent(terms, N, G, r_s.at[N], top)
    for k in range(1, N + 1):
        @pl.when((b < k) & even)
        def _():
            share(k).wait_send()
            if k < N:
                grad_pair(k).wait_send()
        if k > 1:
            @pl.when((b < k) & odd)
            def _():
                share_pair(k).wait_send()

        @pl.when((b + k >= B) & paired(k))
        def _():
            out_grad(k).wait_send()

    @pl.when(w == ROOT)
    def _():
        for d in range(1, W):
            bias_copy(d).wait_send()

    @pl.when(w != ROOT)
    def _():
        bias_copy(1).wait_recv()

    gb_ref[...] = gb[...]


def weight_kernel(x_ref, pg_ref, recon_ref, gb_ref, grad_ref, recon_out, gb_out):
    grad_ref[...] = lax.dot_general(
        x_ref[...], pg_ref[...], (((0,), (0,)), ((), ())), preferred_element_type=F32
    ).astype(BF)
    recon_out[...] = recon_ref[...]
    gb_out[...] = gb_ref[...]


def on_device(B, W, inputs, encoder, enc_bias, active_blocks, near_decoders, far_decoders, targets):
    N = B // 2
    x = inputs[0]
    tok, width = x.shape
    feats = encoder.shape[2]
    half = far_decoders.shape[1]
    out_cols = targets.shape[2]
    C = min(half, 256)
    G = feats // C
    dma = pltpu.SemaphoreType.DMA
    blocks = lambda *lead: pltpu.VMEM((*lead, tok, C), BF)
    rows = lambda *lead: pltpu.VMEM((*lead, tok, out_cols), BF)
    vmem = pl.BlockSpec(memory_space=pltpu.VMEM)
    hbm = pl.BlockSpec(memory_space=pl.ANY)
    recon, pre_grad, bias_sum = pl.pallas_call(
        functools.partial(step_kernel, B, W, C, feats // active_blocks.shape[2]),
        out_shape=(jax.ShapeDtypeStruct((tok, out_cols), F32), jax.ShapeDtypeStruct((tok, feats), BF),
                   jax.ShapeDtypeStruct((1, feats), F32)),
        in_specs=[hbm] * 7,
        out_specs=(vmem, vmem, vmem),
        scratch_shapes=[
            pltpu.VMEM((tok, width), BF),
            pltpu.VMEM((1, feats), F32),
            pltpu.VMEM((active_blocks.shape[2], tok), active_blocks.dtype),
            pltpu.VMEM((tok, out_cols), BF),
            pltpu.VMEM((width, feats), BF),
            pltpu.VMEM((N, feats, out_cols), BF),
            pltpu.VMEM((half, out_cols), BF),
            blocks(4, G), blocks(4, G), blocks(N + 1, G),
            pltpu.VMEM((N + 1, tok, out_cols), F32),
            rows(N + 1), rows(N + 1), rows(N + 1),
            blocks(N + 1, G), blocks(N - 2, G), blocks(N + 1, G), blocks(G),
            pltpu.VMEM((G, tok, C), F32),
            pltpu.VMEM((tok, feats), BF),
            pltpu.VMEM((1, feats), F32),
            dma((4,)), dma((min(G, 4),)), dma((N,)), dma,
            dma((4,)), dma((4, G)),
            dma((N + 1,)), dma((N + 1,)), dma((N, G)),
            dma((N + 1,)), dma((N + 1,)), dma((N + 1,)), dma((N + 1,)),
            dma((N + 1,)), dma((N - 2, G)), dma((N + 1,)), dma((N, G)),
            dma, dma((G,)), dma((W,)), dma,
        ],
        compiler_params=pltpu.CompilerParams(
            collective_id=0, has_side_effects=True, vmem_limit_bytes=67_000_000),
        name="step",
    )(x, encoder[0], enc_bias, active_blocks[0].T, near_decoders[0], far_decoders[0], targets[0])
    steps = max(1, feats // 2048)
    tile = feats // steps
    part = tok // steps
    enc_grad, recon, bias_grad = pl.pallas_call(
        weight_kernel,
        grid=(steps,),
        out_shape=(jax.ShapeDtypeStruct((width, feats), BF), jax.ShapeDtypeStruct((tok, out_cols), F32),
                   jax.ShapeDtypeStruct((1, feats), F32)),
        in_specs=[pl.BlockSpec((tok, width), lambda i: (0, 0)), pl.BlockSpec((tok, tile), lambda i: (0, i)),
                  pl.BlockSpec((part, out_cols), lambda i: (i, 0)), pl.BlockSpec((1, tile), lambda i: (0, i))],
        out_specs=(pl.BlockSpec((width, tile), lambda i: (0, i)), pl.BlockSpec((part, out_cols), lambda i: (i, 0)),
                   pl.BlockSpec((1, tile), lambda i: (0, i))),
        name="weights",
    )(x, pre_grad, recon, bias_sum)
    return recon[None], enc_grad[None], bias_grad


def solution(mesh):
    return jax.shard_map(
        functools.partial(on_device, mesh.shape["blk"], mesh.shape["width"]),
        mesh=mesh,
        in_specs=(
            P("blk", None, "width"),
            P("blk", "width", None),
            P("blk", None),
            P("blk", None, None),
            P("blk", None, None, "width"),
            P("blk", None, "width"),
            P("blk", None, "width"),
        ),
        out_specs=(P("blk", None, "width"), P("blk", "width", None), P("blk", None)),
        check_vma=False,
    )
```
